8 devices in a mesh: dep: 2 (over z, y), col: 2 (over x), row: 2 (over core).
Axes of the slice: x: 2, y: 2, z: 1, core: 2. Of those that a mesh axis runs over, the one named last changes fastest.
Arguments:
- a_mat: bfloat16 [3072, 3072], P('row', 'col')
- b_mat: bfloat16 [3072, 3072], P('row', 'col')
Outputs:
- output: float32 [3072, 3072], P('row', ('col', 'dep'))
All inputs are finite; a program needn't handle non-finite values.
Results may differ from the reference program's by a relative error of at most 0.001.
Values are sent between devices in bfloat16 or wider.
A program may use at most 1 GiB of HBM per device.

```python
import jax
import jax.numpy as jnp

N = 3072


def setup_inputs(seed: int = 0) -> dict:
    key = jax.random.key(seed)
    key_a, key_b = jax.random.split(key)
    a_mat = (jax.random.normal(key_a, (N, N), jnp.float32) * N ** -0.5).astype(jnp.bfloat16)
    b_mat = jax.random.normal(key_b, (N, N), jnp.float32).astype(jnp.bfloat16)
    return {"a_mat": a_mat, "b_mat": b_mat}


def reference(a_mat, b_mat):
    return jnp.dot(a_mat, b_mat, preferred_element_type=jnp.float32)
```

```python
import functools

import jax
import jax.numpy as jnp
from jax import lax
from jax.experimental import pallas as pl
from jax.experimental.pallas import tpu as pltpu
from jax.sharding import PartitionSpec as P

MESH = pl.DeviceIdType.MESH
CHUNK = 32
LEAD = 2


def kernel(n_x, n_y, a_hbm, b_hbm, c_ref, a_loc, a_rem, b_full, a_sem, b_sem, x_send, x_recv, y_send, y_recv, d_send, d_recv):
    layer = lax.axis_index('dep')
    col = lax.axis_index('col')
    row = lax.axis_index('row')
    rows = a_loc.shape[0]
    width = b_full.shape[2]
    rest = rows - n_x * CHUNK

    def place(owner, idx):
        start = idx * CHUNK + owner * (rows - (2 * idx + 1) * CHUNK)
        return pl.ds(pl.multiple_of(start, CHUNK), CHUNK)

    def load_a(idx):
        sl = place(layer, idx)
        return pltpu.make_async_copy(a_hbm.at[sl], a_loc.at[sl], a_sem.at[idx])

    rest_sl = pl.ds(pl.multiple_of((1 - layer) * n_x * CHUNK, CHUNK), rest)
    load_rest = pltpu.make_async_copy(a_hbm.at[rest_sl], a_loc.at[rest_sl], a_sem.at[n_x])
    load_b = pltpu.make_async_copy(b_hbm.at[:, pl.ds(pl.multiple_of(layer * width, 128), width)], b_full.at[row], b_sem)

    def send_x(idx):
        sl = place(layer, idx)
        return pltpu.make_async_remote_copy(
            src_ref=a_loc.at[sl], dst_ref=a_rem.at[sl], send_sem=x_send.at[idx], recv_sem=x_recv.at[idx],
            device_id=(layer, 1 - col, row), device_id_type=MESH)

    def send_y(idx):
        sl = place(layer, idx)
        return pltpu.make_async_remote_copy(
            src_ref=a_rem.at[sl], dst_ref=a_rem.at[sl], send_sem=y_send.at[idx], recv_sem=y_recv.at[idx],
            device_id=(1 - layer, col, row), device_id_type=MESH)

    def recv_y(idx):
        sl = place(1 - layer, idx)
        return pltpu.make_async_remote_copy(
            src_ref=a_rem.at[sl], dst_ref=a_rem.at[sl], send_sem=y_send.at[idx], recv_sem=y_recv.at[idx],
            device_id=(1 - layer, col, row), device_id_type=MESH)

    def swap_b(half):
        return pltpu.make_async_remote_copy(
            src_ref=b_full.at[half], dst_ref=b_full.at[half], send_sem=d_send, recv_sem=d_recv,
            device_id=(layer, col, 1 - row), device_id_type=MESH)

    lax.fori_loop(0, n_x, lambda i, u: (load_a(i).start(), u)[1], 0)
    load_b.start()
    load_rest.start()

    barrier = pltpu.get_barrier_semaphore()
    for peer in ((layer, 1 - col, row), (1 - layer, col, row), (layer, col, 1 - row)):
        pl.semaphore_signal(barrier, inc=1, device_id=peer, device_id_type=MESH)
    pl.semaphore_wait(barrier, 3)

    def launch(i, u):
        load_a(i).wait()
        send_x(i).start()
        return u

    lax.fori_loop(0, n_x, launch, 0)
    load_b.wait()
    swap_b(row).start()
    load_rest.wait()
    swap_b(1 - row).wait_recv()

    def local(sl):
        c_ref[sl, :] = jnp.dot(a_loc[sl, :], b_full[col], preferred_element_type=jnp.float32)

    def remote(sl):
        c_ref[sl, :] += jnp.dot(a_rem[sl, :], b_full[1 - col], preferred_element_type=jnp.float32)

    def step(i, u):
        local(place(layer, i))
        send_x(i).wait_recv()

        @pl.when(i < n_y)
        def _():
            send_y(i).start()
            local(place(1 - layer, i))

        remote(place(layer, i))

        @pl.when(i >= LEAD)
        def _():
            recv_y(i - LEAD).wait_recv()
            remote(place(1 - layer, i - LEAD))

        return u

    lax.fori_loop(0, n_x, step, 0)

    lax.fori_loop(0, n_x, lambda i, u: (send_x(i).wait_send(), u)[1], 0)
    lax.fori_loop(0, n_y, lambda i, u: (send_y(i).wait_send(), u)[1], 0)
    swap_b(row).wait_send()


def solution(mesh):
    n_dep = mesh.shape['dep']

    def local_product(a_blk, b_blk):
        rows, depth = a_blk.shape
        width = b_blk.shape[1] // n_dep
        n_x = (rows // CHUNK + LEAD) // 2
        n_y = n_x - LEAD
        return pl.pallas_call(
            functools.partial(kernel, n_x, n_y),
            out_shape=pltpu.VMEM((rows, width), jnp.float32),
            in_specs=[pl.BlockSpec(memory_space=pltpu.HBM)] * 2,
            out_specs=pl.BlockSpec(memory_space=pltpu.VMEM),
            scratch_shapes=[
                pltpu.VMEM((rows, depth), jnp.bfloat16),
                pltpu.VMEM((rows, depth), jnp.bfloat16),
                pltpu.VMEM((2, depth, width), jnp.bfloat16),
                pltpu.SemaphoreType.DMA((n_x + 1,)),
                pltpu.SemaphoreType.DMA,
                pltpu.SemaphoreType.DMA((n_x,)),
                pltpu.SemaphoreType.DMA((n_x,)),
                pltpu.SemaphoreType.DMA((n_y,)),
                pltpu.SemaphoreType.DMA((n_y,)),
                pltpu.SemaphoreType.DMA,
                pltpu.SemaphoreType.DMA,
            ],
            compiler_params=pltpu.CompilerParams(collective_id=0, has_side_effects=True, vmem_limit_bytes=40 * 1024 * 1024),
            name='gather_dot',
        )(pltpu.with_memory_space_constraint(a_blk, pltpu.HBM), pltpu.with_memory_space_constraint(b_blk, pltpu.HBM))

    return jax.shard_map(local_product, mesh=mesh, in_specs=(P('row', 'col'), P('row', 'col')), out_specs=P('row', ('col', 'dep')), check_vma=False)
```

```python
import functools

import jax
import jax.numpy as jnp
from jax import lax
from jax.experimental import pallas as pl
from jax.experimental.pallas import tpu as pltpu
from jax.sharding import PartitionSpec as P

MESH = pl.DeviceIdType.MESH
CHUNK = 16
GROUP = 4
LEAD = 4
HEAD = 4
NEXT = 16
BLOCK = 256
WARM = 6


def kernel(n_x, n_y, a_hbm, b_hbm, c_ref, a_loc, a_rem, b_full, a_sem, b_sem, x_send, x_recv, y_send, y_recv, d_send, d_recv, y_ready, d_ready):
    layer = lax.axis_index('dep')
    col = lax.axis_index('col')
    row = lax.axis_index('row')
    rows = a_loc.shape[0]
    width = b_full.shape[2]
    x_peer = (layer, 1 - col, row)
    y_peer = (1 - layer, col, row)
    d_peer = (layer, col, 1 - row)

    barrier = pltpu.get_barrier_semaphore()
    pl.semaphore_signal(barrier, inc=1, device_id=x_peer, device_id_type=MESH)

    @pl.when(layer == 0)
    def _():
        pl.semaphore_signal(barrier, inc=1, device_id=y_peer, device_id_type=MESH)

    @pl.when(row == 1)
    def _():
        pl.semaphore_signal(barrier, inc=1, device_id=d_peer, device_id_type=MESH)

    def place(owner, idx, count):
        start = idx * CHUNK + owner * (rows - (2 * idx + count) * CHUNK)
        return pl.ds(pl.multiple_of(start, CHUNK), count * CHUNK)

    def load_a(idx, count, sem):
        sl = place(layer, idx, count)
        return pltpu.make_async_copy(a_hbm.at[sl], a_loc.at[sl], a_sem.at[sem])

    loads = [load_a(i, 1, i) for i in range(HEAD)]
    loads.append(load_a(HEAD, NEXT - HEAD, HEAD))
    loads.append(load_a(NEXT, rows // CHUNK - NEXT, HEAD + 1))
    load_b = pltpu.make_async_copy(b_hbm.at[:, pl.ds(pl.multiple_of(layer * width, 128), width)], b_full.at[row], b_sem)

    def send_x(idx):
        sl = place(layer, idx, 1)
        return pltpu.make_async_remote_copy(
            src_ref=a_loc.at[sl], dst_ref=a_rem.at[sl], send_sem=x_send.at[idx], recv_sem=x_recv.at[idx],
            device_id=x_peer, device_id_type=MESH)

    def copy_y(owner, idx):
        sl = place(owner, idx, 1)
        return pltpu.make_async_remote_copy(
            src_ref=a_rem.at[sl], dst_ref=a_rem.at[sl], send_sem=y_send.at[idx], recv_sem=y_recv.at[idx],
            device_id=y_peer, device_id_type=MESH)

    def swap_b(half):
        return pltpu.make_async_remote_copy(
            src_ref=b_full.at[half], dst_ref=b_full.at[half], send_sem=d_send, recv_sem=d_recv,
            device_id=d_peer, device_id_type=MESH)

    for copy in loads[:HEAD + 1]:
        copy.start()
    load_b.start()
    loads[HEAD + 1].start()

    pl.semaphore_wait(barrier, 2 + layer - row)

    for i in range(HEAD):
        loads[i].wait()
        send_x(i).start()

    @pl.when(layer == 1)
    def _():
        pl.semaphore_signal(y_ready, inc=1, device_id=y_peer, device_id_type=MESH)

    @pl.when(row == 0)
    def _():
        pl.semaphore_signal(d_ready, inc=1, device_id=d_peer, device_id_type=MESH)

    def launch(i, u):
        send_x(i).start()
        return u

    loads[HEAD].wait()
    lax.fori_loop(HEAD, NEXT, launch, 0)
    load_b.wait()

    @pl.when(row == 1)
    def _():
        pl.semaphore_wait(d_ready, 1)

    swap_b(row).start()
    loads[HEAD + 1].wait()
    lax.fori_loop(NEXT, n_x, launch, 0)

    @pl.when(layer == 0)
    def _():
        pl.semaphore_wait(y_ready, 1)

    def remote(sl):
        c_ref[sl, :] += jnp.dot(a_rem[sl, :], b_full[1 - col], preferred_element_type=jnp.float32)

    n_local = rows // BLOCK
    join = WARM + n_local
    g_x = n_x // GROUP
    g_y = n_y // GROUP

    def step(i, u):
        @pl.when(i < n_x)
        def _():
            send_x(i).wait_recv()

        @pl.when(i < n_y)
        def _():
            copy_y(layer, i).start()

        @pl.when(i == WARM)
        def _():
            swap_b(1 - row).wait_recv()

        @pl.when((i >= WARM) & (i < join))
        def _():
            sl = pl.ds(pl.multiple_of((i - WARM) * BLOCK, BLOCK), BLOCK)
            c_ref[sl, :] = jnp.dot(a_loc[sl, :], b_full[col], preferred_element_type=jnp.float32)

        first_y = join + GROUP
        x_turn = jnp.where(i < first_y, i - join, jnp.where(i % GROUP == GROUP - 1, i // GROUP, -1))
        x_turn = jnp.where((i < first_y) | (i >= first_y + GROUP - 1), x_turn, -1)
        y_turn = jnp.where(i < first_y + GROUP - 1, i - first_y, jnp.where(i % GROUP == 0, i // GROUP - 2, -1))
        is_x = (x_turn >= 0) & (x_turn < g_x)
        is_y = (y_turn >= 0) & (y_turn < g_y)

        @pl.when(is_y)
        def _():
            for k in range(GROUP):
                copy_y(1 - layer, y_turn * GROUP + k).wait_recv()

        @pl.when(is_x | is_y)
        def _():
            owner = jnp.where(is_x, layer, 1 - layer)
            remote(place(owner, jnp.where(is_x, x_turn, y_turn) * GROUP, GROUP))

        return u

    lax.fori_loop(0, max(n_x, (g_y + 1) * GROUP + 1), step, 0)

    for k in range(g_y * GROUP, n_y):
        copy_y(1 - layer, k).wait_recv()
    if n_x % GROUP:
        remote(place(layer, g_x * GROUP, GROUP))

    lax.fori_loop(0, n_x, lambda i, u: (send_x(i).wait_send(), u)[1], 0)
    lax.fori_loop(0, n_y, lambda i, u: (copy_y(layer, i).wait_send(), u)[1], 0)
    swap_b(row).wait_send()


def solution(mesh):
    n_dep = mesh.shape['dep']

    def local_product(a_blk, b_blk):
        rows, depth = a_blk.shape
        width = b_blk.shape[1] // n_dep
        n_x = (rows // CHUNK + LEAD) // 2
        n_y = n_x - LEAD
        return pl.pallas_call(
            functools.partial(kernel, n_x, n_y),
            out_shape=pltpu.VMEM((rows, width), jnp.float32),
            in_specs=[pl.BlockSpec(memory_space=pltpu.HBM)] * 2,
            out_specs=pl.BlockSpec(memory_space=pltpu.VMEM),
            scratch_shapes=[
                pltpu.VMEM((rows, depth), jnp.bfloat16),
                pltpu.VMEM((rows, depth), jnp.bfloat16),
                pltpu.VMEM((2, depth, width), jnp.bfloat16),
                pltpu.SemaphoreType.DMA((HEAD + 2,)),
                pltpu.SemaphoreType.DMA,
                pltpu.SemaphoreType.DMA((n_x,)),
                pltpu.SemaphoreType.DMA((n_x,)),
                pltpu.SemaphoreType.DMA((n_y,)),
                pltpu.SemaphoreType.DMA((n_y,)),
                pltpu.SemaphoreType.DMA,
                pltpu.SemaphoreType.DMA,
                pltpu.SemaphoreType.REGULAR,
                pltpu.SemaphoreType.REGULAR,
            ],
            compiler_params=pltpu.CompilerParams(collective_id=0, has_side_effects=True, vmem_limit_bytes=40 * 1024 * 1024),
            name='gather_dot',
        )(pltpu.with_memory_space_constraint(a_blk, pltpu.HBM), pltpu.with_memory_space_constraint(b_blk, pltpu.HBM))

    return jax.shard_map(local_product, mesh=mesh, in_specs=(P('row', 'col'), P('row', 'col')), out_specs=P('row', ('col', 'dep')), check_vma=False)
```

```python
import functools

import jax
import jax.numpy as jnp
from jax import lax
from jax.experimental import pallas as pl
from jax.experimental.pallas import tpu as pltpu
from jax.sharding import PartitionSpec as P

MESH = pl.DeviceIdType.MESH
CHUNK = 32
GROUP = 64 // CHUNK
LEAD = 64 // CHUNK
LAG = 80 // CHUNK
HEAD = 64 // CHUNK
NEXT = 256 // CHUNK
BLOCK = 256
WARM = 96 // CHUNK


def kernel(n_x, n_y, a_hbm, b_hbm, c_ref, a_loc, a_rem, b_full, a_sem, b_sem, x_send, x_recv, y_send, y_recv, d_send, d_recv, y_ready, d_ready):
    layer = lax.axis_index('dep')
    col = lax.axis_index('col')
    row = lax.axis_index('row')
    rows = a_loc.shape[0]
    width = b_full.shape[2]
    x_peer = (layer, 1 - col, row)
    y_peer = (1 - layer, col, row)
    d_peer = (layer, col, 1 - row)

    barrier = pltpu.get_barrier_semaphore()
    pl.semaphore_signal(barrier, inc=1, device_id=x_peer, device_id_type=MESH)

    @pl.when(layer == 0)
    def _():
        pl.semaphore_signal(barrier, inc=1, device_id=y_peer, device_id_type=MESH)

    @pl.when(row == 1)
    def _():
        pl.semaphore_signal(barrier, inc=1, device_id=d_peer, device_id_type=MESH)

    def place(owner, idx, count):
        start = idx * CHUNK + owner * (rows - (2 * idx + count) * CHUNK)
        return pl.ds(pl.multiple_of(start, CHUNK), count * CHUNK)

    def load_a(idx, count, sem):
        sl = place(layer, idx, count)
        return pltpu.make_async_copy(a_hbm.at[sl], a_loc.at[sl], a_sem.at[sem])

    loads = [load_a(i, 1, i) for i in range(HEAD)]
    loads.append(load_a(HEAD, NEXT - HEAD, HEAD))
    loads.append(load_a(NEXT, rows // CHUNK - NEXT, HEAD + 1))
    load_b = pltpu.make_async_copy(b_hbm.at[:, pl.ds(pl.multiple_of(layer * width, 128), width)], b_full.at[row], b_sem)

    def send_x(idx):
        sl = place(layer, idx, 1)
        return pltpu.make_async_remote_copy(
            src_ref=a_loc.at[sl], dst_ref=a_rem.at[sl], send_sem=x_send.at[idx], recv_sem=x_recv.at[idx],
            device_id=x_peer, device_id_type=MESH)

    def copy_y(owner, idx):
        sl = place(owner, idx, 1)
        return pltpu.make_async_remote_copy(
            src_ref=a_rem.at[sl], dst_ref=a_rem.at[sl], send_sem=y_send.at[idx], recv_sem=y_recv.at[idx],
            device_id=y_peer, device_id_type=MESH)

    def swap_b(half):
        return pltpu.make_async_remote_copy(
            src_ref=b_full.at[half], dst_ref=b_full.at[half], send_sem=d_send, recv_sem=d_recv,
            device_id=d_peer, device_id_type=MESH)

    for copy in loads[:HEAD + 1]:
        copy.start()
    load_b.start()
    loads[HEAD + 1].start()

    pl.semaphore_wait(barrier, 2 + layer - row)

    for i in range(HEAD):
        loads[i].wait()
        send_x(i).start()

    @pl.when(layer == 1)
    def _():
        pl.semaphore_signal(y_ready, inc=1, device_id=y_peer, device_id_type=MESH)

    @pl.when(row == 0)
    def _():
        pl.semaphore_signal(d_ready, inc=1, device_id=d_peer, device_id_type=MESH)

    def launch(i, u):
        send_x(i).start()
        return u

    loads[HEAD].wait()
    lax.fori_loop(HEAD, NEXT, launch, 0)
    load_b.wait()

    @pl.when(row == 1)
    def _():
        pl.semaphore_wait(d_ready, 1)

    swap_b(row).start()
    loads[HEAD + 1].wait()
    lax.fori_loop(NEXT, n_x, launch, 0)

    @pl.when(layer == 0)
    def _():
        pl.semaphore_wait(y_ready, 1)

    def remote(sl):
        c_ref[sl, :] += jnp.dot(a_rem[sl, :], b_full[1 - col], preferred_element_type=jnp.float32)

    join = WARM + rows // BLOCK
    g_x = n_x // GROUP
    g_y = n_y // GROUP

    def step(i, done):
        x_done, y_done = done

        @pl.when(i < n_x)
        def _():
            send_x(i).wait_recv()

        @pl.when(i < n_y)
        def _():
            copy_y(layer, i).start()

        @pl.when(i == WARM)
        def _():
            swap_b(1 - row).wait_recv()

        @pl.when((i >= WARM) & (i < join))
        def _():
            sl = pl.ds(pl.multiple_of((i - WARM) * BLOCK, BLOCK), BLOCK)
            c_ref[sl, :] = jnp.dot(a_loc[sl, :], b_full[col], preferred_element_type=jnp.float32)

        is_x = (i >= join) & (x_done < g_x) & ((x_done + 1) * GROUP <= i + 1)
        is_y = (i >= join) & (y_done < g_y) & ((y_done + 1) * GROUP + LAG <= i + 1)

        @pl.when(is_x)
        def _():
            remote(place(layer, x_done * GROUP, GROUP))

        @pl.when(is_y)
        def _():
            for k in range(GROUP):
                copy_y(1 - layer, y_done * GROUP + k).wait_recv()
            remote(place(1 - layer, y_done * GROUP, GROUP))

        return x_done + is_x.astype(jnp.int32), y_done + is_y.astype(jnp.int32)

    lax.fori_loop(0, max(n_x, g_y * GROUP + LAG), step, (0, 0))

    for k in range(g_y * GROUP, n_y):
        copy_y(1 - layer, k).wait_recv()
    if n_x % GROUP:
        remote(place(layer, g_x * GROUP, GROUP))

    lax.fori_loop(0, n_x, lambda i, u: (send_x(i).wait_send(), u)[1], 0)
    lax.fori_loop(0, n_y, lambda i, u: (copy_y(layer, i).wait_send(), u)[1], 0)
    swap_b(row).wait_send()


def solution(mesh):
    n_dep = mesh.shape['dep']

    def local_product(a_blk, b_blk):
        rows, depth = a_blk.shape
        width = b_blk.shape[1] // n_dep
        n_x = (rows // CHUNK + LEAD) // 2
        n_y = n_x - LEAD
        return pl.pallas_call(
            functools.partial(kernel, n_x, n_y),
            out_shape=pltpu.VMEM((rows, width), jnp.float32),
            in_specs=[pl.BlockSpec(memory_space=pltpu.HBM)] * 2,
            out_specs=pl.BlockSpec(memory_space=pltpu.VMEM),
            scratch_shapes=[
                pltpu.VMEM((rows, depth), jnp.bfloat16),
                pltpu.VMEM((rows, depth), jnp.bfloat16),
                pltpu.VMEM((2, depth, width), jnp.bfloat16),
                pltpu.SemaphoreType.DMA((HEAD + 2,)),
                pltpu.SemaphoreType.DMA,
                pltpu.SemaphoreType.DMA((n_x,)),
                pltpu.SemaphoreType.DMA((n_x,)),
                pltpu.SemaphoreType.DMA((n_y,)),
                pltpu.SemaphoreType.DMA((n_y,)),
                pltpu.SemaphoreType.DMA,
                pltpu.SemaphoreType.DMA,
                pltpu.SemaphoreType.REGULAR,
                pltpu.SemaphoreType.REGULAR,
            ],
            compiler_params=pltpu.CompilerParams(collective_id=0, has_side_effects=True, vmem_limit_bytes=40 * 1024 * 1024),
            name='gather_dot',
        )(pltpu.with_memory_space_constraint(a_blk, pltpu.HBM), pltpu.with_memory_space_constraint(b_blk, pltpu.HBM))

    return jax.shard_map(local_product, mesh=mesh, in_specs=(P('row', 'col'), P('row', 'col')), out_specs=P('row', ('col', 'dep')), check_vma=False)
```

```python
import jax
import jax.numpy as jnp
from jax import lax
from jax.experimental import pallas as pl
from jax.experimental.pallas import tpu as pltpu
from jax.sharding import PartitionSpec as P

TAKE = (((26, 26), (24, 24)), ((26, 26), (24, 24)))
MESH = pl.DeviceIdType.MESH
CHUNK = 32
GROUP = 64 // CHUNK
LAG = 80 // CHUNK
HEAD = 64 // CHUNK
NEXT = 256 // CHUNK
BLOCK = 256
WARM = 96 // CHUNK


def taken(layer, col, row):
    total = 0
    for l in range(2):
        for j in range(2):
            for i in range(2):
                total += TAKE[l][j][i] * (l * layer + (1 - l) * (1 - layer)) * (j * col + (1 - j) * (1 - col)) * (i * row + (1 - i) * (1 - row))
    return total


def kernel(a_hbm, b_hbm, c_ref, a_loc, a_rem, b_full, a_sem, b_sem, x_send, x_recv, y_send, y_recv, d_send, d_recv, y_ready, d_ready):
    layer = lax.axis_index('dep')
    col = lax.axis_index('col')
    row = lax.axis_index('row')
    rows = a_loc.shape[0]
    width = b_full.shape[2]
    chunks = rows // CHUNK
    n_x = taken(layer, col, row)
    n_y = chunks - n_x
    n_out = taken(layer, 1 - col, row)
    n_pass = chunks - taken(1 - layer, col, row)
    x_peer = (layer, 1 - col, row)
    y_peer = (1 - layer, col, row)
    d_peer = (layer, col, 1 - row)

    barrier = pltpu.get_barrier_semaphore()
    pl.semaphore_signal(barrier, inc=1, device_id=x_peer, device_id_type=MESH)

    @pl.when(layer == 0)
    def _():
        pl.semaphore_signal(barrier, inc=1, device_id=y_peer, device_id_type=MESH)

    @pl.when(row == 1)
    def _():
        pl.semaphore_signal(barrier, inc=1, device_id=d_peer, device_id_type=MESH)

    def place(owner, idx, count):
        start = idx * CHUNK + owner * (rows - (2 * idx + count) * CHUNK)
        return pl.ds(pl.multiple_of(start, CHUNK), count * CHUNK)

    def load_a(idx, count, sem):
        sl = place(layer, idx, count)
        return pltpu.make_async_copy(a_hbm.at[sl], a_loc.at[sl], a_sem.at[sem])

    loads = [load_a(i, 1, i) for i in range(HEAD)]
    loads.append(load_a(HEAD, NEXT - HEAD, HEAD))
    loads.append(load_a(NEXT, rows // CHUNK - NEXT, HEAD + 1))
    load_b = pltpu.make_async_copy(b_hbm.at[:, pl.ds(pl.multiple_of(layer * width, 128), width)], b_full.at[row], b_sem)

    def send_x(idx):
        sl = place(layer, idx, 1)
        return pltpu.make_async_remote_copy(
            src_ref=a_loc.at[sl], dst_ref=a_rem.at[sl], send_sem=x_send.at[idx], recv_sem=x_recv.at[idx],
            device_id=x_peer, device_id_type=MESH)

    def copy_y(owner, idx):
        sl = place(owner, idx, 1)
        return pltpu.make_async_remote_copy(
            src_ref=a_rem.at[sl], dst_ref=a_rem.at[sl], send_sem=y_send.at[idx], recv_sem=y_recv.at[idx],
            device_id=y_peer, device_id_type=MESH)

    def swap_b(half):
        return pltpu.make_async_remote_copy(
            src_ref=b_full.at[half], dst_ref=b_full.at[half], send_sem=d_send, recv_sem=d_recv,
            device_id=d_peer, device_id_type=MESH)

    for copy in loads[:HEAD + 1]:
        copy.start()
    load_b.start()
    loads[HEAD + 1].start()

    pl.semaphore_wait(barrier, 2 + layer - row)

    for i in range(HEAD):
        loads[i].wait()
        send_x(i).start()

    @pl.when(layer == 1)
    def _():
        pl.semaphore_signal(y_ready, inc=1, device_id=y_peer, device_id_type=MESH)

    @pl.when(row == 0)
    def _():
        pl.semaphore_signal(d_ready, inc=1, device_id=d_peer, device_id_type=MESH)

    def launch(i, u):
        send_x(i).start()
        return u

    loads[HEAD].wait()
    lax.fori_loop(HEAD, NEXT, launch, 0)
    load_b.wait()

    @pl.when(row == 1)
    def _():
        pl.semaphore_wait(d_ready, 1)

    swap_b(row).start()
    loads[HEAD + 1].wait()
    lax.fori_loop(NEXT, n_out, launch, 0)

    @pl.when(layer == 0)
    def _():
        pl.semaphore_wait(y_ready, 1)

    def remote(sl):
        c_ref[sl, :] += jnp.dot(a_rem[sl, :], b_full[1 - col], preferred_element_type=jnp.float32)

    join = WARM + rows // BLOCK
    g_x = n_x // GROUP
    g_y = n_y // GROUP

    def step(i, done):
        x_done, y_done = done

        @pl.when(i < n_x)
        def _():
            send_x(i).wait_recv()

        @pl.when(i < n_pass)
        def _():
            copy_y(layer, i).start()

        @pl.when(i == WARM)
        def _():
            swap_b(1 - row).wait_recv()

        @pl.when((i >= WARM) & (i < join))
        def _():
            sl = pl.ds(pl.multiple_of((i - WARM) * BLOCK, BLOCK), BLOCK)
            c_ref[sl, :] = jnp.dot(a_loc[sl, :], b_full[col], preferred_element_type=jnp.float32)

        is_x = (i >= join) & (x_done < g_x) & ((x_done + 1) * GROUP <= i + 1)
        is_y = (i >= join) & (y_done < g_y) & ((y_done + 1) * GROUP + LAG <= i + 1)

        @pl.when(is_x)
        def _():
            remote(place(layer, x_done * GROUP, GROUP))

        @pl.when(is_y)
        def _():
            for k in range(GROUP):
                copy_y(1 - layer, y_done * GROUP + k).wait_recv()
            remote(place(1 - layer, y_done * GROUP, GROUP))

        return x_done + is_x.astype(jnp.int32), y_done + is_y.astype(jnp.int32)

    lax.fori_loop(0, jnp.maximum(n_x, g_y * GROUP + LAG), step, (0, 0))

    lax.fori_loop(g_y * GROUP, n_y, lambda i, u: (copy_y(1 - layer, i).wait_recv(), u)[1], 0)

    @pl.when(g_x + g_y < chunks // GROUP)
    def _():
        remote(place(layer, g_x * GROUP, GROUP))

    lax.fori_loop(0, n_out, lambda i, u: (send_x(i).wait_send(), u)[1], 0)
    lax.fori_loop(0, n_pass, lambda i, u: (copy_y(layer, i).wait_send(), u)[1], 0)
    swap_b(row).wait_send()


def solution(mesh):
    n_dep = mesh.shape['dep']

    def local_product(a_blk, b_blk):
        rows, depth = a_blk.shape
        width = b_blk.shape[1] // n_dep
        chunks = rows // CHUNK
        return pl.pallas_call(
            kernel,
            out_shape=pltpu.VMEM((rows, width), jnp.float32),
            in_specs=[pl.BlockSpec(memory_space=pltpu.HBM)] * 2,
            out_specs=pl.BlockSpec(memory_space=pltpu.VMEM),
            scratch_shapes=[
                pltpu.VMEM((rows, depth), jnp.bfloat16),
                pltpu.VMEM((rows, depth), jnp.bfloat16),
                pltpu.VMEM((2, depth, width), jnp.bfloat16),
                pltpu.SemaphoreType.DMA((HEAD + 2,)),
                pltpu.SemaphoreType.DMA,
                pltpu.SemaphoreType.DMA((chunks,)),
                pltpu.SemaphoreType.DMA((chunks,)),
                pltpu.SemaphoreType.DMA((chunks,)),
                pltpu.SemaphoreType.DMA((chunks,)),
                pltpu.SemaphoreType.DMA,
                pltpu.SemaphoreType.DMA,
                pltpu.SemaphoreType.REGULAR,
                pltpu.SemaphoreType.REGULAR,
            ],
            compiler_params=pltpu.CompilerParams(collective_id=0, has_side_effects=True, vmem_limit_bytes=40 * 1024 * 1024),
            name='gather_dot',
        )(pltpu.with_memory_space_constraint(a_blk, pltpu.HBM), pltpu.with_memory_space_constraint(b_blk, pltpu.HBM))

    return jax.shard_map(local_product, mesh=mesh, in_specs=(P('row', 'col'), P('row', 'col')), out_specs=P('row', ('col', 'dep')), check_vma=False)
```

```python
import jax
import jax.numpy as jnp
from jax import lax
from jax.experimental import pallas as pl
from jax.experimental.pallas import tpu as pltpu
from jax.sharding import PartitionSpec as P

TAKE = (((24, 25), (24, 25)), ((24, 25), (24, 25)))
MESH = pl.DeviceIdType.MESH
CHUNK = 32
GROUP = 64 // CHUNK
LAG = 80 // CHUNK
HEAD = 64 // CHUNK
NEXT = 256 // CHUNK
BLOCK = 256
LEFT = 5
WARM = 96 // CHUNK


def taken(layer, col, row):
    total = 0
    for l in range(2):
        for j in range(2):
            for i in range(2):
                total += TAKE[l][j][i] * (l * layer + (1 - l) * (1 - layer)) * (j * col + (1 - j) * (1 - col)) * (i * row + (1 - i) * (1 - row))
    return total


def kernel(a_hbm, b_hbm, c_ref, a_loc, a_rem, b_full, a_sem, b_sem, x_send, x_recv, y_send, y_recv, d_send, d_recv, y_ready, d_ready, go):
    layer = lax.axis_index('dep')
    col = lax.axis_index('col')
    row = lax.axis_index('row')
    rows = a_loc.shape[0]
    width = b_full.shape[2]
    chunks = rows // CHUNK
    n_x = taken(layer, col, row)
    n_y = chunks - n_x
    n_out = taken(layer, 1 - col, row)
    n_pass = chunks - taken(1 - layer, col, row)
    x_peer = (layer, 1 - col, row)
    y_peer = (1 - layer, col, row)
    d_peer = (layer, col, 1 - row)

    barrier = pltpu.get_barrier_semaphore()
    pl.semaphore_signal(barrier, inc=1, device_id=x_peer, device_id_type=MESH)

    @pl.when(layer == 0)
    def _():
        pl.semaphore_signal(barrier, inc=1, device_id=y_peer, device_id_type=MESH)

    @pl.when(row == 1)
    def _():
        pl.semaphore_signal(barrier, inc=1, device_id=d_peer, device_id_type=MESH)

    def place(owner, idx, count):
        start = idx * CHUNK + owner * (rows - (2 * idx + count) * CHUNK)
        return pl.ds(pl.multiple_of(start, CHUNK), count * CHUNK)

    def load_a(idx, count, sem):
        sl = place(layer, idx, count)
        return pltpu.make_async_copy(a_hbm.at[sl], a_loc.at[sl], a_sem.at[sem])

    loads = [load_a(i, 1, i) for i in range(HEAD)]
    loads.append(load_a(HEAD, NEXT - HEAD, HEAD))
    loads.append(load_a(NEXT, rows // CHUNK - NEXT, HEAD + 1))
    load_b = pltpu.make_async_copy(b_hbm.at[:, pl.ds(pl.multiple_of(layer * width, 128), width)], b_full.at[row], b_sem)

    def send_x(idx):
        sl = place(layer, idx, 1)
        return pltpu.make_async_remote_copy(
            src_ref=a_loc.at[sl], dst_ref=a_rem.at[sl], send_sem=x_send.at[idx], recv_sem=x_recv.at[idx],
            device_id=x_peer, device_id_type=MESH)

    def copy_y(owner, idx):
        sl = place(owner, idx, 1)
        return pltpu.make_async_remote_copy(
            src_ref=a_rem.at[sl], dst_ref=a_rem.at[sl], send_sem=y_send.at[idx], recv_sem=y_recv.at[idx],
            device_id=y_peer, device_id_type=MESH)

    def swap_b(half):
        return pltpu.make_async_remote_copy(
            src_ref=b_full.at[half], dst_ref=b_full.at[half], send_sem=d_send, recv_sem=d_recv,
            device_id=d_peer, device_id_type=MESH)

    for copy in loads[:HEAD + 1]:
        copy.start()
    load_b.start()
    loads[HEAD + 1].start()

    pl.semaphore_wait(barrier, 2 + layer - row)

    for i in range(HEAD):
        loads[i].wait()

        @pl.when(row == 0)
        def _():
            send_x(i).start()

    @pl.when(layer == 1)
    def _():
        pl.semaphore_signal(y_ready, inc=1, device_id=y_peer, device_id_type=MESH)

    @pl.when(row == 0)
    def _():
        pl.semaphore_signal(d_ready, inc=1, device_id=d_peer, device_id_type=MESH)

    def launch(i, u):
        send_x(i).start()
        return u

    loads[HEAD].wait()

    @pl.when(row == 0)
    def _():
        lax.fori_loop(HEAD, NEXT, launch, 0)

    load_b.wait()

    @pl.when(row == 1)
    def _():
        pl.semaphore_wait(d_ready, 1)

    swap_b(row).start()
    loads[HEAD + 1].wait()

    @pl.when(row == 0)
    def _():
        lax.fori_loop(NEXT, n_out, launch, 0)

    @pl.when(row == 1)
    def _():
        pl.semaphore_wait(go, 1)
        lax.fori_loop(0, n_out, launch, 0)

    @pl.when(layer == 0)
    def _():
        pl.semaphore_wait(y_ready, 1)

    def remote(sl):
        c_ref[sl, :] += jnp.dot(a_rem[sl, :], b_full[1 - col], preferred_element_type=jnp.float32)

    join = WARM + rows // BLOCK
    g_x = n_x // GROUP
    g_y = n_y // GROUP

    def step(i, done):
        x_done, y_done = done

        @pl.when(i < n_x)
        def _():
            send_x(i).wait_recv()

        @pl.when(i < n_pass)
        def _():
            copy_y(layer, i).start()

        @pl.when((i == n_x - LEFT) & (row == 0))
        def _():
            pl.semaphore_signal(go, inc=1, device_id=d_peer, device_id_type=MESH)

        @pl.when(i == WARM)
        def _():
            swap_b(1 - row).wait_recv()

        @pl.when((i >= WARM) & (i < join))
        def _():
            sl = pl.ds(pl.multiple_of((i - WARM) * BLOCK, BLOCK), BLOCK)
            c_ref[sl, :] = jnp.dot(a_loc[sl, :], b_full[col], preferred_element_type=jnp.float32)

        is_x = (i >= join) & (x_done < g_x) & ((x_done + 1) * GROUP <= i + 1)
        is_y = (i >= join) & (y_done < g_y) & ((y_done + 1) * GROUP + LAG <= i + 1)

        @pl.when(is_x)
        def _():
            remote(place(layer, x_done * GROUP, GROUP))

        @pl.when(is_y)
        def _():
            for k in range(GROUP):
                copy_y(1 - layer, y_done * GROUP + k).wait_recv()
            remote(place(1 - layer, y_done * GROUP, GROUP))

        return x_done + is_x.astype(jnp.int32), y_done + is_y.astype(jnp.int32)

    lax.fori_loop(0, jnp.maximum(n_x, g_y * GROUP + LAG), step, (0, 0))

    lax.fori_loop(g_y * GROUP, n_y, lambda i, u: (copy_y(1 - layer, i).wait_recv(), u)[1], 0)

    @pl.when(g_x + g_y < chunks // GROUP)
    def _():
        remote(place(layer, g_x * GROUP, GROUP))

    lax.fori_loop(0, n_out, lambda i, u: (send_x(i).wait_send(), u)[1], 0)
    lax.fori_loop(0, n_pass, lambda i, u: (copy_y(layer, i).wait_send(), u)[1], 0)
    swap_b(row).wait_send()


def solution(mesh):
    n_dep = mesh.shape['dep']

    def local_product(a_blk, b_blk):
        rows, depth = a_blk.shape
        width = b_blk.shape[1] // n_dep
        chunks = rows // CHUNK
        return pl.pallas_call(
            kernel,
            out_shape=pltpu.VMEM((rows, width), jnp.float32),
            in_specs=[pl.BlockSpec(memory_space=pltpu.HBM)] * 2,
            out_specs=pl.BlockSpec(memory_space=pltpu.VMEM),
            scratch_shapes=[
                pltpu.VMEM((rows, depth), jnp.bfloat16),
                pltpu.VMEM((rows, depth), jnp.bfloat16),
                pltpu.VMEM((2, depth, width), jnp.bfloat16),
                pltpu.SemaphoreType.DMA((HEAD + 2,)),
                pltpu.SemaphoreType.DMA,
                pltpu.SemaphoreType.DMA((chunks,)),
                pltpu.SemaphoreType.DMA((chunks,)),
                pltpu.SemaphoreType.DMA((chunks,)),
                pltpu.SemaphoreType.DMA((chunks,)),
                pltpu.SemaphoreType.DMA,
                pltpu.SemaphoreType.DMA,
                pltpu.SemaphoreType.REGULAR,
                pltpu.SemaphoreType.REGULAR,
                pltpu.SemaphoreType.REGULAR,
            ],
            compiler_params=pltpu.CompilerParams(collective_id=0, has_side_effects=True, vmem_limit_bytes=40 * 1024 * 1024),
            name='gather_dot',
        )(pltpu.with_memory_space_constraint(a_blk, pltpu.HBM), pltpu.with_memory_space_constraint(b_blk, pltpu.HBM))

    return jax.shard_map(local_product, mesh=mesh, in_specs=(P('row', 'col'), P('row', 'col')), out_specs=P('row', ('col', 'dep')), check_vma=False)
```

```python
import jax
import jax.numpy as jnp
from jax import lax
from jax.experimental import pallas as pl
from jax.experimental.pallas import tpu as pltpu
from jax.sharding import PartitionSpec as P

TAKE = (((25, 25), (25, 25)), ((25, 25), (25, 25)))
MESH = pl.DeviceIdType.MESH
CHUNK = 32
GROUP = 64 // CHUNK
LAG = 80 // CHUNK
HEAD = 64 // CHUNK
NEXT = 256 // CHUNK
BLOCK = 256
HOLD = 12
WARM = 96 // CHUNK


def taken(layer, col, row):
    total = 0
    for l in range(2):
        for j in range(2):
            for i in range(2):
                total += TAKE[l][j][i] * (l * layer + (1 - l) * (1 - layer)) * (j * col + (1 - j) * (1 - col)) * (i * row + (1 - i) * (1 - row))
    return total


def kernel(a_hbm, b_hbm, c_ref, a_loc, a_rem, b_full, a_sem, b_sem, x_send, x_recv, y_send, y_recv, d_send, d_recv, y_ready, d_ready):
    layer = lax.axis_index('dep')
    col = lax.axis_index('col')
    row = lax.axis_index('row')
    rows = a_loc.shape[0]
    width = b_full.shape[2]
    chunks = rows // CHUNK
    n_x = taken(layer, col, row)
    n_y = chunks - n_x
    n_out = taken(layer, 1 - col, row)
    n_pass = chunks - taken(1 - layer, col, row)
    x_peer = (layer, 1 - col, row)
    y_peer = (1 - layer, col, row)
    d_peer = (layer, col, 1 - row)

    barrier = pltpu.get_barrier_semaphore()
    pl.semaphore_signal(barrier, inc=1, device_id=x_peer, device_id_type=MESH)

    @pl.when(layer == 0)
    def _():
        pl.semaphore_signal(barrier, inc=1, device_id=y_peer, device_id_type=MESH)

    @pl.when(row == 1)
    def _():
        pl.semaphore_signal(barrier, inc=1, device_id=d_peer, device_id_type=MESH)

    def place(owner, idx, count):
        start = idx * CHUNK + owner * (rows - (2 * idx + count) * CHUNK)
        return pl.ds(pl.multiple_of(start, CHUNK), count * CHUNK)

    def load_a(idx, count, sem):
        sl = place(layer, idx, count)
        return pltpu.make_async_copy(a_hbm.at[sl], a_loc.at[sl], a_sem.at[sem])

    loads = [load_a(i, 1, i) for i in range(HEAD)]
    loads.append(load_a(HEAD, NEXT - HEAD, HEAD))
    loads.append(load_a(NEXT, rows // CHUNK - NEXT, HEAD + 1))
    load_b = pltpu.make_async_copy(b_hbm.at[:, pl.ds(pl.multiple_of(layer * width, 128), width)], b_full.at[row], b_sem)

    def send_x(idx):
        sl = place(layer, idx, 1)
        return pltpu.make_async_remote_copy(
            src_ref=a_loc.at[sl], dst_ref=a_rem.at[sl], send_sem=x_send.at[idx], recv_sem=x_recv.at[idx],
            device_id=x_peer, device_id_type=MESH)

    def copy_y(owner, idx):
        sl = place(owner, idx, 1)
        return pltpu.make_async_remote_copy(
            src_ref=a_rem.at[sl], dst_ref=a_rem.at[sl], send_sem=y_send.at[idx], recv_sem=y_recv.at[idx],
            device_id=y_peer, device_id_type=MESH)

    def swap_b(half):
        return pltpu.make_async_remote_copy(
            src_ref=b_full.at[half], dst_ref=b_full.at[half], send_sem=d_send, recv_sem=d_recv,
            device_id=d_peer, device_id_type=MESH)

    for copy in loads[:HEAD + 1]:
        copy.start()
    load_b.start()
    loads[HEAD + 1].start()

    pl.semaphore_wait(barrier, 2 + layer - row)

    for i in range(HEAD):
        loads[i].wait()
        send_x(i).start()

    @pl.when(layer == 1)
    def _():
        pl.semaphore_signal(y_ready, inc=1, device_id=y_peer, device_id_type=MESH)

    @pl.when(row == 0)
    def _():
        pl.semaphore_signal(d_ready, inc=1, device_id=d_peer, device_id_type=MESH)

    def launch(i, u):
        send_x(i).start()
        return u

    loads[HEAD].wait()
    lax.fori_loop(HEAD, NEXT, launch, 0)
    load_b.wait()

    @pl.when(row == 1)
    def _():
        pl.semaphore_wait(d_ready, 1)

    swap_b(row).start()
    loads[HEAD + 1].wait()
    first_out = jnp.where(row == 0, n_out, HOLD)
    lax.fori_loop(NEXT, first_out, launch, 0)

    @pl.when(layer == 0)
    def _():
        pl.semaphore_wait(y_ready, 1)

    def remote(sl):
        c_ref[sl, :] += jnp.dot(a_rem[sl, :], b_full[1 - col], preferred_element_type=jnp.float32)

    join = WARM + rows // BLOCK
    g_x = n_x // GROUP
    g_y = n_y // GROUP

    def step(i, done):
        x_done, y_done = done

        @pl.when(i < n_x)
        def _():
            send_x(i).wait_recv()

        @pl.when(i < n_pass)
        def _():
            copy_y(layer, i).start()

        @pl.when(i == HOLD - 1)
        def _():
            lax.fori_loop(first_out, n_out, launch, 0)

        @pl.when(i == WARM)
        def _():
            swap_b(1 - row).wait_recv()

        @pl.when((i >= WARM) & (i < join))
        def _():
            sl = pl.ds(pl.multiple_of((i - WARM) * BLOCK, BLOCK), BLOCK)
            c_ref[sl, :] = jnp.dot(a_loc[sl, :], b_full[col], preferred_element_type=jnp.float32)

        is_x = (i >= join) & (x_done < g_x) & ((x_done + 1) * GROUP <= i + 1)
        is_y = (i >= join) & (y_done < g_y) & ((y_done + 1) * GROUP + LAG <= i + 1)

        @pl.when(is_x)
        def _():
            remote(place(layer, x_done * GROUP, GROUP))

        @pl.when(is_y)
        def _():
            for k in range(GROUP):
                copy_y(1 - layer, y_done * GROUP + k).wait_recv()
            remote(place(1 - layer, y_done * GROUP, GROUP))

        return x_done + is_x.astype(jnp.int32), y_done + is_y.astype(jnp.int32)

    lax.fori_loop(0, jnp.maximum(n_x, g_y * GROUP + LAG), step, (0, 0))

    lax.fori_loop(g_y * GROUP, n_y, lambda i, u: (copy_y(1 - layer, i).wait_recv(), u)[1], 0)

    @pl.when(g_x + g_y < chunks // GROUP)
    def _():
        remote(place(layer, g_x * GROUP, GROUP))

    lax.fori_loop(0, n_out, lambda i, u: (send_x(i).wait_send(), u)[1], 0)
    lax.fori_loop(0, n_pass, lambda i, u: (copy_y(layer, i).wait_send(), u)[1], 0)
    swap_b(row).wait_send()


def solution(mesh):
    n_dep = mesh.shape['dep']

    def local_product(a_blk, b_blk):
        rows, depth = a_blk.shape
        width = b_blk.shape[1] // n_dep
        chunks = rows // CHUNK
        return pl.pallas_call(
            kernel,
            out_shape=pltpu.VMEM((rows, width), jnp.float32),
            in_specs=[pl.BlockSpec(memory_space=pltpu.HBM)] * 2,
            out_specs=pl.BlockSpec(memory_space=pltpu.VMEM),
            scratch_shapes=[
                pltpu.VMEM((rows, depth), jnp.bfloat16),
                pltpu.VMEM((rows, depth), jnp.bfloat16),
                pltpu.VMEM((2, depth, width), jnp.bfloat16),
                pltpu.SemaphoreType.DMA((HEAD + 2,)),
                pltpu.SemaphoreType.DMA,
                pltpu.SemaphoreType.DMA((chunks,)),
                pltpu.SemaphoreType.DMA((chunks,)),
                pltpu.SemaphoreType.DMA((chunks,)),
                pltpu.SemaphoreType.DMA((chunks,)),
                pltpu.SemaphoreType.DMA,
                pltpu.SemaphoreType.DMA,
                pltpu.SemaphoreType.REGULAR,
                pltpu.SemaphoreType.REGULAR,
            ],
            compiler_params=pltpu.CompilerParams(collective_id=0, has_side_effects=True, vmem_limit_bytes=40 * 1024 * 1024),
            name='gather_dot',
        )(pltpu.with_memory_space_constraint(a_blk, pltpu.HBM), pltpu.with_memory_space_constraint(b_blk, pltpu.HBM))

    return jax.shard_map(local_product, mesh=mesh, in_specs=(P('row', 'col'), P('row', 'col')), out_specs=P('row', ('col', 'dep')), check_vma=False)
```

```python
import jax
import jax.numpy as jnp
from jax import lax
from jax.experimental import pallas as pl
from jax.experimental.pallas import tpu as pltpu
from jax.sharding import PartitionSpec as P

MESH = pl.DeviceIdType.MESH
FIRST = 16
CHUNK = 32
GROUP = 2
LAG = 2
HEAD = 3
NEXT = 9
BLOCK = 256
WARM = 3
TAKE = (26, 25)


def kernel(a_hbm, b_hbm, c_ref, a_loc, a_rem, b_full, stage, a_sem, b_sem, x_send, x_recv, y_send, y_recv,
           d_send, d_recv, s_send, s_recv, h_send, y_ready, d_ready):
    layer = lax.axis_index('dep')
    col = lax.axis_index('col')
    row = lax.axis_index('row')
    rows = a_loc.shape[0]
    width = b_full.shape[2]
    copies = rows // CHUNK + 1
    n_x = jnp.where(row == 0, TAKE[0], TAKE[1])
    n_y = copies - n_x
    n_own = jnp.where(row == 0, TAKE[0] - 1, TAKE[1])
    x_peer = (layer, 1 - col, row)
    y_peer = (1 - layer, col, row)
    d_peer = (layer, col, 1 - row)

    barrier = pltpu.get_barrier_semaphore()
    pl.semaphore_signal(barrier, inc=1, device_id=x_peer, device_id_type=MESH)

    @pl.when(layer == 0)
    def _():
        pl.semaphore_signal(barrier, inc=1, device_id=y_peer, device_id_type=MESH)

    @pl.when(row == 1)
    def _():
        pl.semaphore_signal(barrier, inc=1, device_id=d_peer, device_id_type=MESH)

    def span(owner, start, count):
        return pl.ds(pl.multiple_of(start + owner * (rows - 2 * start - count), FIRST), count)

    def place(owner, idx):
        if isinstance(idx, int) and idx == 0:
            return span(owner, 0, FIRST)
        return span(owner, FIRST + (idx - 1) * CHUNK, CHUNK)

    def load_a(start, stop, sem):
        sl = span(layer, start, stop - start)
        return pltpu.make_async_copy(a_hbm.at[sl], a_loc.at[sl], a_sem.at[sem])

    ends = [FIRST + i * CHUNK for i in range(HEAD)] + [FIRST + (NEXT - 1) * CHUNK, rows]
    loads = [load_a(start, stop, sem) for sem, (start, stop) in enumerate(zip([0] + ends, ends))]
    load_b = pltpu.make_async_copy(b_hbm.at[:, pl.ds(pl.multiple_of(layer * width, 128), width)], b_full.at[row], b_sem)

    def send_x(idx):
        sl = place(layer, idx)
        return pltpu.make_async_remote_copy(
            src_ref=a_loc.at[sl], dst_ref=a_rem.at[sl], send_sem=x_send.at[idx], recv_sem=x_recv.at[idx],
            device_id=x_peer, device_id_type=MESH)

    def copy_y(owner, idx):
        sl = place(owner, idx)
        return pltpu.make_async_remote_copy(
            src_ref=a_rem.at[sl], dst_ref=a_rem.at[sl], send_sem=y_send.at[idx], recv_sem=y_recv.at[idx],
            device_id=y_peer, device_id_type=MESH)

    def swap_b(half):
        return pltpu.make_async_remote_copy(
            src_ref=b_full.at[half], dst_ref=b_full.at[half], send_sem=d_send, recv_sem=d_recv,
            device_id=d_peer, device_id_type=MESH)

    helped = TAKE[0] - 1
    hand = pltpu.make_async_remote_copy(
        src_ref=a_hbm.at[place(layer, helped)], dst_ref=stage, send_sem=s_send, recv_sem=s_recv,
        device_id=d_peer, device_id_type=MESH)
    send_help = pltpu.make_async_remote_copy(
        src_ref=stage, dst_ref=a_rem.at[place(layer, helped)], send_sem=h_send, recv_sem=x_recv.at[helped],
        device_id=(layer, 1 - col, 0), device_id_type=MESH)

    for copy in loads[:-1]:
        copy.start()
    load_b.start()
    loads[-1].start()

    pl.semaphore_wait(barrier, 2 + layer - row)

    for i in range(HEAD):
        loads[i].wait()
        send_x(i).start()

    @pl.when(layer == 1)
    def _():
        pl.semaphore_signal(y_ready, inc=1, device_id=y_peer, device_id_type=MESH)

    @pl.when(row == 0)
    def _():
        pl.semaphore_signal(d_ready, inc=1, device_id=d_peer, device_id_type=MESH)

    def launch(i, u):
        send_x(i).start()
        return u

    loads[HEAD].wait()
    lax.fori_loop(HEAD, NEXT, launch, 0)
    load_b.wait()

    @pl.when(row == 1)
    def _():
        pl.semaphore_wait(d_ready, 1)

    swap_b(row).start()

    @pl.when(row == 0)
    def _():
        hand.start()

    loads[-1].wait()
    lax.fori_loop(NEXT, n_own - 1, launch, 0)

    @pl.when(row == 1)
    def _():
        hand.wait_recv()
        send_help.start()

    send_x(n_own - 1).start()

    @pl.when(layer == 0)
    def _():
        pl.semaphore_wait(y_ready, 1)

    def remote(sl):
        c_ref[sl, :] += jnp.dot(a_rem[sl, :], b_full[1 - col], preferred_element_type=jnp.float32)

    def group(owner, idx):
        return span(owner, FIRST + idx * GROUP * CHUNK, GROUP * CHUNK)

    join = WARM + rows // BLOCK
    g_x = (n_x - 2) // GROUP
    g_y = (n_y - 2) // GROUP

    send_x(0).wait_recv()
    copy_y(layer, 0).start()

    def step(i, done):
        x_done, y_done = done

        @pl.when(i < n_x)
        def _():
            send_x(i).wait_recv()

        @pl.when(i < n_y)
        def _():
            copy_y(layer, i).start()

        @pl.when(i == WARM)
        def _():
            swap_b(1 - row).wait_recv()

        @pl.when((i >= WARM) & (i < join))
        def _():
            sl = pl.ds(pl.multiple_of((i - WARM) * BLOCK, BLOCK), BLOCK)
            c_ref[sl, :] = jnp.dot(a_loc[sl, :], b_full[col], preferred_element_type=jnp.float32)

        @pl.when(i == join)
        def _():
            remote(place(layer, 0))
            copy_y(1 - layer, 0).wait_recv()
            remote(place(1 - layer, 0))

        is_x = (i > join) & (x_done < g_x) & ((x_done + 1) * GROUP <= i)
        is_y = (i > join) & (y_done < g_y) & ((y_done + 1) * GROUP + LAG <= i)

        @pl.when(is_x)
        def _():
            remote(group(layer, x_done))

        @pl.when(is_y)
        def _():
            for k in range(GROUP):
                copy_y(1 - layer, y_done * GROUP + k + 1).wait_recv()
            remote(group(1 - layer, y_done))

        return x_done + is_x.astype(jnp.int32), y_done + is_y.astype(jnp.int32)

    lax.fori_loop(1, jnp.maximum(n_x, g_y * GROUP + LAG + 1), step, (0, 0))

    lax.fori_loop(g_y * GROUP + 1, n_y, lambda i, u: (copy_y(1 - layer, i).wait_recv(), u)[1], 0)
    left = rows - 2 * FIRST - sum((t - 2) // GROUP * GROUP * CHUNK for t in (TAKE[0], copies - TAKE[0]))
    remote(span(layer, FIRST + g_x * GROUP * CHUNK, left))

    send_x(0).wait_send()
    copy_y(layer, 0).wait_send()
    lax.fori_loop(1, n_own, lambda i, u: (send_x(i).wait_send(), u)[1], 0)
    lax.fori_loop(1, n_y, lambda i, u: (copy_y(layer, i).wait_send(), u)[1], 0)
    swap_b(row).wait_send()

    @pl.when(row == 0)
    def _():
        hand.wait_send()

    @pl.when(row == 1)
    def _():
        send_help.wait_send()


def solution(mesh):
    n_dep = mesh.shape['dep']

    def local_product(a_blk, b_blk):
        rows, depth = a_blk.shape
        width = b_blk.shape[1] // n_dep
        copies = rows // CHUNK + 1
        return pl.pallas_call(
            kernel,
            out_shape=pltpu.VMEM((rows, width), jnp.float32),
            in_specs=[pl.BlockSpec(memory_space=pltpu.HBM)] * 2,
            out_specs=pl.BlockSpec(memory_space=pltpu.VMEM),
            scratch_shapes=[
                pltpu.VMEM((rows, depth), jnp.bfloat16),
                pltpu.VMEM((rows, depth), jnp.bfloat16),
                pltpu.VMEM((2, depth, width), jnp.bfloat16),
                pltpu.VMEM((CHUNK, depth), jnp.bfloat16),
                pltpu.SemaphoreType.DMA((HEAD + 2,)),
                pltpu.SemaphoreType.DMA,
                pltpu.SemaphoreType.DMA((copies,)),
                pltpu.SemaphoreType.DMA((copies,)),
                pltpu.SemaphoreType.DMA((copies,)),
                pltpu.SemaphoreType.DMA((copies,)),
                pltpu.SemaphoreType.DMA,
                pltpu.SemaphoreType.DMA,
                pltpu.SemaphoreType.DMA,
                pltpu.SemaphoreType.DMA,
                pltpu.SemaphoreType.DMA,
                pltpu.SemaphoreType.REGULAR,
                pltpu.SemaphoreType.REGULAR,
            ],
            compiler_params=pltpu.CompilerParams(collective_id=0, has_side_effects=True, vmem_limit_bytes=40 * 1024 * 1024),
            name='gather_dot',
        )(pltpu.with_memory_space_constraint(a_blk, pltpu.HBM), pltpu.with_memory_space_constraint(b_blk, pltpu.HBM))

    return jax.shard_map(local_product, mesh=mesh, in_specs=(P('row', 'col'), P('row', 'col')), out_specs=P('row', ('col', 'dep')), check_vma=False)
```

```python
import functools

import jax
import jax.numpy as jnp
from jax import lax
from jax.experimental import pallas as pl
from jax.experimental.pallas import tpu as pltpu
from jax.sharding import PartitionSpec as P

MESH = pl.DeviceIdType.MESH
CHUNK = 32
GROUP = 64 // CHUNK
LEAD = 64 // CHUNK
LAG = 80 // CHUNK
HEAD = 64 // CHUNK
NEXT = 256 // CHUNK
BLOCK = 256
WARM = 96 // CHUNK


def kernel(n_x, n_y, a_hbm, b_hbm, c_ref, a_loc, a_rem, b_full, a_sem, b_sem, x_send, x_recv, y_send, y_recv, d_send, d_recv, y_ready, d_ready):
    layer = lax.axis_index('dep')
    col = lax.axis_index('col')
    row = lax.axis_index('row')
    rows = a_loc.shape[0]
    width = b_full.shape[2]
    x_peer = (layer, 1 - col, row)
    y_peer = (1 - layer, col, row)
    d_peer = (layer, col, 1 - row)

    barrier = pltpu.get_barrier_semaphore()
    pl.semaphore_signal(barrier, inc=1, device_id=x_peer, device_id_type=MESH)

    @pl.when(layer == 0)
    def _():
        pl.semaphore_signal(barrier, inc=1, device_id=y_peer, device_id_type=MESH)

    @pl.when(row == 1)
    def _():
        pl.semaphore_signal(barrier, inc=1, device_id=d_peer, device_id_type=MESH)

    def place(owner, idx, count):
        start = idx * CHUNK + owner * (rows - (2 * idx + count) * CHUNK)
        return pl.ds(pl.multiple_of(start, CHUNK), count * CHUNK)

    def load_a(idx, count, sem):
        sl = place(layer, idx, count)
        return pltpu.make_async_copy(a_hbm.at[sl], a_loc.at[sl], a_sem.at[sem])

    loads = [load_a(i, 1, i) for i in range(HEAD)]
    loads.append(load_a(HEAD, NEXT - HEAD, HEAD))
    loads.append(load_a(NEXT, rows // CHUNK - NEXT, HEAD + 1))
    load_b = pltpu.make_async_copy(b_hbm.at[:, pl.ds(pl.multiple_of(layer * width, 128), width)], b_full.at[row], b_sem)

    def send_x(idx):
        sl = place(layer, idx, 1)
        return pltpu.make_async_remote_copy(
            src_ref=a_hbm.at[sl], dst_ref=a_rem.at[sl], send_sem=x_send.at[idx], recv_sem=x_recv.at[idx],
            device_id=x_peer, device_id_type=MESH)

    def copy_y(owner, idx):
        sl = place(owner, idx, 1)
        return pltpu.make_async_remote_copy(
            src_ref=a_rem.at[sl], dst_ref=a_rem.at[sl], send_sem=y_send.at[idx], recv_sem=y_recv.at[idx],
            device_id=y_peer, device_id_type=MESH)

    def swap_b(half):
        return pltpu.make_async_remote_copy(
            src_ref=b_full.at[half], dst_ref=b_full.at[half], send_sem=d_send, recv_sem=d_recv,
            device_id=d_peer, device_id_type=MESH)

    for copy in loads[:HEAD + 1]:
        copy.start()
    load_b.start()
    loads[HEAD + 1].start()

    pl.semaphore_wait(barrier, 2 + layer - row)

    for i in range(HEAD):
        send_x(i).start()

    @pl.when(layer == 1)
    def _():
        pl.semaphore_signal(y_ready, inc=1, device_id=y_peer, device_id_type=MESH)

    @pl.when(row == 0)
    def _():
        pl.semaphore_signal(d_ready, inc=1, device_id=d_peer, device_id_type=MESH)

    def launch(i, u):
        send_x(i).start()
        return u

    lax.fori_loop(HEAD, n_x, launch, 0)
    load_b.wait()

    @pl.when(row == 1)
    def _():
        pl.semaphore_wait(d_ready, 1)

    swap_b(row).start()
    for copy in loads:
        copy.wait()

    @pl.when(layer == 0)
    def _():
        pl.semaphore_wait(y_ready, 1)

    def remote(sl):
        c_ref[sl, :] += jnp.dot(a_rem[sl, :], b_full[1 - col], preferred_element_type=jnp.float32)

    join = WARM + rows // BLOCK
    g_x = n_x // GROUP
    g_y = n_y // GROUP

    def step(i, done):
        x_done, y_done = done

        @pl.when(i < n_x)
        def _():
            send_x(i).wait_recv()

        @pl.when(i < n_y)
        def _():
            copy_y(layer, i).start()

        @pl.when(i == WARM)
        def _():
            swap_b(1 - row).wait_recv()

        @pl.when((i >= WARM) & (i < join))
        def _():
            sl = pl.ds(pl.multiple_of((i - WARM) * BLOCK, BLOCK), BLOCK)
            c_ref[sl, :] = jnp.dot(a_loc[sl, :], b_full[col], preferred_element_type=jnp.float32)

        is_x = (i >= join) & (x_done < g_x) & ((x_done + 1) * GROUP <= i + 1)
        is_y = (i >= join) & (y_done < g_y) & ((y_done + 1) * GROUP + LAG <= i + 1)

        @pl.when(is_x)
        def _():
            remote(place(layer, x_done * GROUP, GROUP))

        @pl.when(is_y)
        def _():
            for k in range(GROUP):
                copy_y(1 - layer, y_done * GROUP + k).wait_recv()
            remote(place(1 - layer, y_done * GROUP, GROUP))

        return x_done + is_x.astype(jnp.int32), y_done + is_y.astype(jnp.int32)

    lax.fori_loop(0, max(n_x, g_y * GROUP + LAG), step, (0, 0))

    for k in range(g_y * GROUP, n_y):
        copy_y(1 - layer, k).wait_recv()
    if n_x % GROUP:
        remote(place(layer, g_x * GROUP, GROUP))

    lax.fori_loop(0, n_x, lambda i, u: (send_x(i).wait_send(), u)[1], 0)
    lax.fori_loop(0, n_y, lambda i, u: (copy_y(layer, i).wait_send(), u)[1], 0)
    swap_b(row).wait_send()


def solution(mesh):
    n_dep = mesh.shape['dep']

    def local_product(a_blk, b_blk):
        rows, depth = a_blk.shape
        width = b_blk.shape[1] // n_dep
        n_x = (rows // CHUNK + LEAD) // 2
        n_y = n_x - LEAD
        return pl.pallas_call(
            functools.partial(kernel, n_x, n_y),
            out_shape=pltpu.VMEM((rows, width), jnp.float32),
            in_specs=[pl.BlockSpec(memory_space=pltpu.HBM)] * 2,
            out_specs=pl.BlockSpec(memory_space=pltpu.VMEM),
            scratch_shapes=[
                pltpu.VMEM((rows, depth), jnp.bfloat16),
                pltpu.VMEM((rows, depth), jnp.bfloat16),
                pltpu.VMEM((2, depth, width), jnp.bfloat16),
                pltpu.SemaphoreType.DMA((HEAD + 2,)),
                pltpu.SemaphoreType.DMA,
                pltpu.SemaphoreType.DMA((n_x,)),
                pltpu.SemaphoreType.DMA((n_x,)),
                pltpu.SemaphoreType.DMA((n_y,)),
                pltpu.SemaphoreType.DMA((n_y,)),
                pltpu.SemaphoreType.DMA,
                pltpu.SemaphoreType.DMA,
                pltpu.SemaphoreType.REGULAR,
                pltpu.SemaphoreType.REGULAR,
            ],
            compiler_params=pltpu.CompilerParams(collective_id=0, has_side_effects=True, vmem_limit_bytes=40 * 1024 * 1024),
            name='gather_dot',
        )(pltpu.with_memory_space_constraint(a_blk, pltpu.HBM), pltpu.with_memory_space_constraint(b_blk, pltpu.HBM))

    return jax.shard_map(local_product, mesh=mesh, in_specs=(P('row', 'col'), P('row', 'col')), out_specs=P('row', ('col', 'dep')), check_vma=False)
```

```python
import jax
import jax.numpy as jnp
from jax import lax
from jax.experimental import pallas as pl
from jax.experimental.pallas import tpu as pltpu
from jax.sharding import PartitionSpec as P

MESH = pl.DeviceIdType.MESH
CHUNK = 32
GROUP = 64 // CHUNK
HELP = 1
TAKE = (25 + HELP, 25)
LAG = 80 // CHUNK
HEAD = 64 // CHUNK
NEXT = 256 // CHUNK
BLOCK = 256
WARM = 96 // CHUNK


def kernel(a_hbm, b_hbm, c_ref, a_loc, a_rem, b_full, stage, a_sem, b_sem, x_send, x_recv, y_send, y_recv, d_send, d_recv, s_send, s_recv, h_send, y_ready, d_ready):
    layer = lax.axis_index('dep')
    col = lax.axis_index('col')
    row = lax.axis_index('row')
    rows = a_loc.shape[0]
    width = b_full.shape[2]
    chunks = rows // CHUNK
    n_x = jnp.where(row == 0, TAKE[0], TAKE[1])
    n_y = chunks - n_x
    n_own = jnp.where(row == 0, TAKE[0] - HELP, TAKE[1])
    x_peer = (layer, 1 - col, row)
    y_peer = (1 - layer, col, row)
    d_peer = (layer, col, 1 - row)

    barrier = pltpu.get_barrier_semaphore()
    pl.semaphore_signal(barrier, inc=1, device_id=x_peer, device_id_type=MESH)

    @pl.when(layer == 0)
    def _():
        pl.semaphore_signal(barrier, inc=1, device_id=y_peer, device_id_type=MESH)

    @pl.when(row == 1)
    def _():
        pl.semaphore_signal(barrier, inc=1, device_id=d_peer, device_id_type=MESH)

    def place(owner, idx, count):
        start = idx * CHUNK + owner * (rows - (2 * idx + count) * CHUNK)
        return pl.ds(pl.multiple_of(start, CHUNK), count * CHUNK)

    def load_a(idx, count, sem):
        sl = place(layer, idx, count)
        return pltpu.make_async_copy(a_hbm.at[sl], a_loc.at[sl], a_sem.at[sem])

    loads = [load_a(i, 1, i) for i in range(HEAD)]
    loads.append(load_a(HEAD, NEXT - HEAD, HEAD))
    loads.append(load_a(NEXT, rows // CHUNK - NEXT, HEAD + 1))
    load_b = pltpu.make_async_copy(b_hbm.at[:, pl.ds(pl.multiple_of(layer * width, 128), width)], b_full.at[row], b_sem)

    def send_x(idx):
        sl = place(layer, idx, 1)
        return pltpu.make_async_remote_copy(
            src_ref=a_hbm.at[sl], dst_ref=a_rem.at[sl], send_sem=x_send.at[idx], recv_sem=x_recv.at[idx],
            device_id=x_peer, device_id_type=MESH)

    def copy_y(owner, idx):
        sl = place(owner, idx, 1)
        return pltpu.make_async_remote_copy(
            src_ref=a_rem.at[sl], dst_ref=a_rem.at[sl], send_sem=y_send.at[idx], recv_sem=y_recv.at[idx],
            device_id=y_peer, device_id_type=MESH)

    def swap_b(half):
        return pltpu.make_async_remote_copy(
            src_ref=b_full.at[half], dst_ref=b_full.at[half], send_sem=d_send, recv_sem=d_recv,
            device_id=d_peer, device_id_type=MESH)

    def hand(k):
        return pltpu.make_async_remote_copy(
            src_ref=a_hbm.at[place(layer, TAKE[0] - HELP + k, 1)], dst_ref=stage.at[k], send_sem=s_send.at[k], recv_sem=s_recv.at[k],
            device_id=d_peer, device_id_type=MESH)

    def send_help(k):
        idx = TAKE[0] - HELP + k
        return pltpu.make_async_remote_copy(
            src_ref=stage.at[k], dst_ref=a_rem.at[place(layer, idx, 1)], send_sem=h_send.at[k], recv_sem=x_recv.at[idx],
            device_id=(layer, 1 - col, 0), device_id_type=MESH)

    for copy in loads[:HEAD + 1]:
        copy.start()
    load_b.start()
    loads[HEAD + 1].start()

    pl.semaphore_wait(barrier, 2 + layer - row)

    for i in range(HEAD):
        send_x(i).start()

    @pl.when(layer == 1)
    def _():
        pl.semaphore_signal(y_ready, inc=1, device_id=y_peer, device_id_type=MESH)

    @pl.when(row == 0)
    def _():
        pl.semaphore_signal(d_ready, inc=1, device_id=d_peer, device_id_type=MESH)

    def launch(i, u):
        send_x(i).start()
        return u

    lax.fori_loop(HEAD, jnp.where(row == 0, n_own, n_y), launch, 0)
    load_b.wait()

    @pl.when(row == 1)
    def _():
        pl.semaphore_wait(d_ready, 1)

    swap_b(row).start()

    @pl.when(row == 0)
    def _():
        for k in range(HELP):
            hand(k).start()

    @pl.when(row == 1)
    def _():
        for k in range(HELP):
            hand(k).wait_recv()
            send_help(k).start()
        lax.fori_loop(n_y, n_own, launch, 0)

    for copy in loads:
        copy.wait()

    @pl.when(layer == 0)
    def _():
        pl.semaphore_wait(y_ready, 1)

    def remote(sl):
        c_ref[sl, :] += jnp.dot(a_rem[sl, :], b_full[1 - col], preferred_element_type=jnp.float32)

    join = WARM + rows // BLOCK
    g_x = n_x // GROUP
    g_y = n_y // GROUP

    def step(i, done):
        x_done, y_done = done

        @pl.when(i < n_x)
        def _():
            send_x(i).wait_recv()

        @pl.when(i < n_y)
        def _():
            copy_y(layer, i).start()

        @pl.when(i == WARM)
        def _():
            swap_b(1 - row).wait_recv()

        @pl.when((i >= WARM) & (i < join))
        def _():
            sl = pl.ds(pl.multiple_of((i - WARM) * BLOCK, BLOCK), BLOCK)
            c_ref[sl, :] = jnp.dot(a_loc[sl, :], b_full[col], preferred_element_type=jnp.float32)

        is_x = (i >= join) & (x_done < g_x) & ((x_done + 1) * GROUP <= i + 1)
        is_y = (i >= join) & (y_done < g_y) & ((y_done + 1) * GROUP + LAG <= i + 1)

        @pl.when(is_x)
        def _():
            remote(place(layer, x_done * GROUP, GROUP))

        @pl.when(is_y)
        def _():
            for k in range(GROUP):
                copy_y(1 - layer, y_done * GROUP + k).wait_recv()
            remote(place(1 - layer, y_done * GROUP, GROUP))

        return x_done + is_x.astype(jnp.int32), y_done + is_y.astype(jnp.int32)

    lax.fori_loop(0, jnp.maximum(n_x, g_y * GROUP + LAG), step, (0, 0))

    lax.fori_loop(g_y * GROUP, n_y, lambda i, u: (copy_y(1 - layer, i).wait_recv(), u)[1], 0)

    @pl.when(g_x + g_y < chunks // GROUP)
    def _():
        remote(place(layer, g_x * GROUP, GROUP))

    lax.fori_loop(0, n_own, lambda i, u: (send_x(i).wait_send(), u)[1], 0)
    lax.fori_loop(0, n_y, lambda i, u: (copy_y(layer, i).wait_send(), u)[1], 0)

    @pl.when(row == 0)
    def _():
        for k in range(HELP):
            hand(k).wait_send()

    @pl.when(row == 1)
    def _():
        for k in range(HELP):
            send_help(k).wait_send()

    swap_b(row).wait_send()


def solution(mesh):
    n_dep = mesh.shape['dep']

    def local_product(a_blk, b_blk):
        rows, depth = a_blk.shape
        width = b_blk.shape[1] // n_dep
        chunks = rows // CHUNK
        return pl.pallas_call(
            kernel,
            out_shape=pltpu.VMEM((rows, width), jnp.float32),
            in_specs=[pl.BlockSpec(memory_space=pltpu.HBM)] * 2,
            out_specs=pl.BlockSpec(memory_space=pltpu.VMEM),
            scratch_shapes=[
                pltpu.VMEM((rows, depth), jnp.bfloat16),
                pltpu.VMEM((rows, depth), jnp.bfloat16),
                pltpu.VMEM((2, depth, width), jnp.bfloat16),
                pltpu.VMEM((HELP, CHUNK, depth), jnp.bfloat16),
                pltpu.SemaphoreType.DMA((HEAD + 2,)),
                pltpu.SemaphoreType.DMA,
                pltpu.SemaphoreType.DMA((chunks,)),
                pltpu.SemaphoreType.DMA((chunks,)),
                pltpu.SemaphoreType.DMA((chunks,)),
                pltpu.SemaphoreType.DMA((chunks,)),
                pltpu.SemaphoreType.DMA,
                pltpu.SemaphoreType.DMA,
                pltpu.SemaphoreType.DMA((HELP,)),
                pltpu.SemaphoreType.DMA((HELP,)),
                pltpu.SemaphoreType.DMA((HELP,)),
                pltpu.SemaphoreType.REGULAR,
                pltpu.SemaphoreType.REGULAR,
            ],
            compiler_params=pltpu.CompilerParams(collective_id=0, has_side_effects=True, vmem_limit_bytes=40 * 1024 * 1024),
            name='gather_dot',
        )(pltpu.with_memory_space_constraint(a_blk, pltpu.HBM), pltpu.with_memory_space_constraint(b_blk, pltpu.HBM))

    return jax.shard_map(local_product, mesh=mesh, in_specs=(P('row', 'col'), P('row', 'col')), out_specs=P('row', ('col', 'dep')), check_vma=False)
```

```python
import functools

import jax
import jax.numpy as jnp
from jax import lax
from jax.experimental import pallas as pl
from jax.experimental.pallas import tpu as pltpu
from jax.sharding import PartitionSpec as P

MESH = pl.DeviceIdType.MESH
CHUNK = 32
GROUP = 64 // CHUNK
LEAD = 64 // CHUNK
LAG = 80 // CHUNK
HEAD = 64 // CHUNK
NEXT = 256 // CHUNK
BLOCK = 256
START = 0
WARM = 96 // CHUNK


def kernel(n_x, n_y, a_hbm, b_hbm, c_ref, a_loc, a_rem, b_full, a_sem, b_sem, x_send, x_recv, y_send, y_recv, d_send, d_recv, y_ready, d_ready, go):
    layer = lax.axis_index('dep')
    col = lax.axis_index('col')
    row = lax.axis_index('row')
    rows = a_loc.shape[0]
    width = b_full.shape[2]
    x_peer = (layer, 1 - col, row)
    y_peer = (1 - layer, col, row)
    d_peer = (layer, col, 1 - row)

    barrier = pltpu.get_barrier_semaphore()
    pl.semaphore_signal(barrier, inc=1, device_id=x_peer, device_id_type=MESH)

    @pl.when(layer == 0)
    def _():
        pl.semaphore_signal(barrier, inc=1, device_id=y_peer, device_id_type=MESH)

    @pl.when(row == 1)
    def _():
        pl.semaphore_signal(barrier, inc=1, device_id=d_peer, device_id_type=MESH)

    def place(owner, idx, count):
        start = idx * CHUNK + owner * (rows - (2 * idx + count) * CHUNK)
        return pl.ds(pl.multiple_of(start, CHUNK), count * CHUNK)

    def load_a(idx, count, sem):
        sl = place(layer, idx, count)
        return pltpu.make_async_copy(a_hbm.at[sl], a_loc.at[sl], a_sem.at[sem])

    loads = [load_a(i, 1, i) for i in range(HEAD)]
    loads.append(load_a(HEAD, NEXT - HEAD, HEAD))
    loads.append(load_a(NEXT, rows // CHUNK - NEXT, HEAD + 1))
    load_b = pltpu.make_async_copy(b_hbm.at[:, pl.ds(pl.multiple_of(layer * width, 128), width)], b_full.at[row], b_sem)

    def send_x(idx):
        sl = place(layer, idx, 1)
        return pltpu.make_async_remote_copy(
            src_ref=a_hbm.at[sl], dst_ref=a_rem.at[sl], send_sem=x_send.at[idx], recv_sem=x_recv.at[idx],
            device_id=x_peer, device_id_type=MESH)

    def copy_y(owner, idx):
        sl = place(owner, idx, 1)
        return pltpu.make_async_remote_copy(
            src_ref=a_rem.at[sl], dst_ref=a_rem.at[sl], send_sem=y_send.at[idx], recv_sem=y_recv.at[idx],
            device_id=y_peer, device_id_type=MESH)

    def swap_b(half):
        return pltpu.make_async_remote_copy(
            src_ref=b_full.at[half], dst_ref=b_full.at[half], send_sem=d_send, recv_sem=d_recv,
            device_id=d_peer, device_id_type=MESH)

    for copy in loads[:HEAD + 1]:
        copy.start()
    load_b.start()
    loads[HEAD + 1].start()

    pl.semaphore_wait(barrier, 2 + layer - row)

    def launch(i, u):
        send_x(i).start()
        return u

    @pl.when(row == 0)
    def _():
        lax.fori_loop(0, n_x, launch, 0)

    @pl.when(layer == 1)
    def _():
        pl.semaphore_signal(y_ready, inc=1, device_id=y_peer, device_id_type=MESH)

    @pl.when(row == 0)
    def _():
        pl.semaphore_signal(d_ready, inc=1, device_id=d_peer, device_id_type=MESH)

    load_b.wait()

    @pl.when(row == 1)
    def _():
        pl.semaphore_wait(d_ready, 1)

    swap_b(row).start()
    for copy in loads:
        copy.wait()

    @pl.when(row == 1)
    def _():
        pl.semaphore_wait(go, 1)
        lax.fori_loop(0, n_x, launch, 0)

    @pl.when(layer == 0)
    def _():
        pl.semaphore_wait(y_ready, 1)

    def remote(sl):
        c_ref[sl, :] += jnp.dot(a_rem[sl, :], b_full[1 - col], preferred_element_type=jnp.float32)

    join = WARM + rows // BLOCK
    g_x = n_x // GROUP
    g_y = n_y // GROUP

    def step(i, done):
        x_done, y_done = done

        @pl.when(i < n_x)
        def _():
            send_x(i).wait_recv()

        @pl.when(i < n_y)
        def _():
            copy_y(layer, i).start()

        @pl.when((i == START) & (row == 0))
        def _():
            pl.semaphore_signal(go, inc=1, device_id=d_peer, device_id_type=MESH)

        @pl.when(i == WARM)
        def _():
            swap_b(1 - row).wait_recv()

        @pl.when((i >= WARM) & (i < join))
        def _():
            sl = pl.ds(pl.multiple_of((i - WARM) * BLOCK, BLOCK), BLOCK)
            c_ref[sl, :] = jnp.dot(a_loc[sl, :], b_full[col], preferred_element_type=jnp.float32)

        is_x = (i >= join) & (x_done < g_x) & ((x_done + 1) * GROUP <= i + 1)
        is_y = (i >= join) & (y_done < g_y) & ((y_done + 1) * GROUP + LAG <= i + 1)

        @pl.when(is_x)
        def _():
            remote(place(layer, x_done * GROUP, GROUP))

        @pl.when(is_y)
        def _():
            for k in range(GROUP):
                copy_y(1 - layer, y_done * GROUP + k).wait_recv()
            remote(place(1 - layer, y_done * GROUP, GROUP))

        return x_done + is_x.astype(jnp.int32), y_done + is_y.astype(jnp.int32)

    lax.fori_loop(0, max(n_x, g_y * GROUP + LAG), step, (0, 0))

    for k in range(g_y * GROUP, n_y):
        copy_y(1 - layer, k).wait_recv()
    if n_x % GROUP:
        remote(place(layer, g_x * GROUP, GROUP))

    lax.fori_loop(0, n_x, lambda i, u: (send_x(i).wait_send(), u)[1], 0)
    lax.fori_loop(0, n_y, lambda i, u: (copy_y(layer, i).wait_send(), u)[1], 0)
    swap_b(row).wait_send()


def solution(mesh):
    n_dep = mesh.shape['dep']

    def local_product(a_blk, b_blk):
        rows, depth = a_blk.shape
        width = b_blk.shape[1] // n_dep
        n_x = (rows // CHUNK + LEAD) // 2
        n_y = n_x - LEAD
        return pl.pallas_call(
            functools.partial(kernel, n_x, n_y),
            out_shape=pltpu.VMEM((rows, width), jnp.float32),
            in_specs=[pl.BlockSpec(memory_space=pltpu.HBM)] * 2,
            out_specs=pl.BlockSpec(memory_space=pltpu.VMEM),
            scratch_shapes=[
                pltpu.VMEM((rows, depth), jnp.bfloat16),
                pltpu.VMEM((rows, depth), jnp.bfloat16),
                pltpu.VMEM((2, depth, width), jnp.bfloat16),
                pltpu.SemaphoreType.DMA((HEAD + 2,)),
                pltpu.SemaphoreType.DMA,
                pltpu.SemaphoreType.DMA((n_x,)),
                pltpu.SemaphoreType.DMA((n_x,)),
                pltpu.SemaphoreType.DMA((n_y,)),
                pltpu.SemaphoreType.DMA((n_y,)),
                pltpu.SemaphoreType.DMA,
                pltpu.SemaphoreType.DMA,
                pltpu.SemaphoreType.REGULAR,
                pltpu.SemaphoreType.REGULAR,
                pltpu.SemaphoreType.REGULAR,
            ],
            compiler_params=pltpu.CompilerParams(collective_id=0, has_side_effects=True, vmem_limit_bytes=40 * 1024 * 1024),
            name='gather_dot',
        )(pltpu.with_memory_space_constraint(a_blk, pltpu.HBM), pltpu.with_memory_space_constraint(b_blk, pltpu.HBM))

    return jax.shard_map(local_product, mesh=mesh, in_specs=(P('row', 'col'), P('row', 'col')), out_specs=P('row', ('col', 'dep')), check_vma=False)
```

```python
import functools

import jax
import jax.numpy as jnp
from jax import lax
from jax.experimental import pallas as pl
from jax.experimental.pallas import tpu as pltpu
from jax.sharding import PartitionSpec as P

MESH = pl.DeviceIdType.MESH
CHUNK = 32
GROUP = 64 // CHUNK
LEAD = 64 // CHUNK
LAG = 128 // CHUNK
HEAD = 64 // CHUNK
NEXT = 256 // CHUNK
BLOCK = 256
START = 1
WARM = 96 // CHUNK


def kernel(n_x, n_y, a_hbm, b_hbm, c_ref, a_loc, a_rem, b_full, a_sem, b_sem, x_send, x_recv, y_send, y_recv, d_send, d_recv, y_ready, d_ready, go):
    layer = lax.axis_index('dep')
    col = lax.axis_index('col')
    row = lax.axis_index('row')
    rows = a_loc.shape[0]
    width = b_full.shape[2]
    x_peer = (layer, 1 - col, row)
    y_peer = (1 - layer, col, row)
    d_peer = (layer, col, 1 - row)

    barrier = pltpu.get_barrier_semaphore()
    pl.semaphore_signal(barrier, inc=1, device_id=x_peer, device_id_type=MESH)

    @pl.when(layer == 0)
    def _():
        pl.semaphore_signal(barrier, inc=1, device_id=y_peer, device_id_type=MESH)

    @pl.when(row == 1)
    def _():
        pl.semaphore_signal(barrier, inc=1, device_id=d_peer, device_id_type=MESH)

    def place(owner, idx, count):
        start = idx * CHUNK + owner * (rows - (2 * idx + count) * CHUNK)
        return pl.ds(pl.multiple_of(start, CHUNK), count * CHUNK)

    def load_a(idx, count, sem):
        sl = place(layer, idx, count)
        return pltpu.make_async_copy(a_hbm.at[sl], a_loc.at[sl], a_sem.at[sem])

    loads = [load_a(i, 1, i) for i in range(HEAD)]
    loads.append(load_a(HEAD, NEXT - HEAD, HEAD))
    loads.append(load_a(NEXT, rows // CHUNK - NEXT, HEAD + 1))
    load_b = pltpu.make_async_copy(b_hbm.at[:, pl.ds(pl.multiple_of(layer * width, 128), width)], b_full.at[row], b_sem)

    def send_x(idx):
        sl = place(layer, idx, 1)
        return pltpu.make_async_remote_copy(
            src_ref=a_hbm.at[sl], dst_ref=a_rem.at[sl], send_sem=x_send.at[idx], recv_sem=x_recv.at[idx],
            device_id=x_peer, device_id_type=MESH)

    def copy_y(owner, idx):
        sl = place(owner, idx, 1)
        return pltpu.make_async_remote_copy(
            src_ref=a_rem.at[sl], dst_ref=a_rem.at[sl], send_sem=y_send.at[idx], recv_sem=y_recv.at[idx],
            device_id=y_peer, device_id_type=MESH)

    def swap_b(half):
        return pltpu.make_async_remote_copy(
            src_ref=b_full.at[half], dst_ref=b_full.at[half], send_sem=d_send, recv_sem=d_recv,
            device_id=d_peer, device_id_type=MESH)

    for copy in loads[:HEAD + 1]:
        copy.start()
    load_b.start()
    loads[HEAD + 1].start()

    pl.semaphore_wait(barrier, 2 + layer - row)

    def launch(i, u):
        send_x(i).start()
        return u

    @pl.when(row == 0)
    def _():
        lax.fori_loop(0, n_x, launch, 0)

    @pl.when(layer == 1)
    def _():
        pl.semaphore_signal(y_ready, inc=1, device_id=y_peer, device_id_type=MESH)

    @pl.when(row == 0)
    def _():
        pl.semaphore_signal(d_ready, inc=1, device_id=d_peer, device_id_type=MESH)

    load_b.wait()

    @pl.when(row == 1)
    def _():
        pl.semaphore_wait(d_ready, 1)

    swap_b(row).start()

    @pl.when(row == 0)
    def _():
        for i in range(START):
            send_x(i).wait_send()
        pl.semaphore_signal(go, inc=1, device_id=d_peer, device_id_type=MESH)

    for copy in loads:
        copy.wait()

    @pl.when(row == 1)
    def _():
        pl.semaphore_wait(go, 1)
        lax.fori_loop(0, n_x, launch, 0)

    @pl.when(layer == 0)
    def _():
        pl.semaphore_wait(y_ready, 1)

    def remote(sl):
        c_ref[sl, :] += jnp.dot(a_rem[sl, :], b_full[1 - col], preferred_element_type=jnp.float32)

    join = WARM + rows // BLOCK
    g_x = n_x // GROUP
    g_y = n_y // GROUP

    def step(i, done):
        x_done, y_done = done

        @pl.when(i < n_x)
        def _():
            send_x(i).wait_recv()

        @pl.when(i < n_y)
        def _():
            copy_y(layer, i).start()

        @pl.when(i == WARM)
        def _():
            swap_b(1 - row).wait_recv()

        @pl.when((i >= WARM) & (i < join))
        def _():
            sl = pl.ds(pl.multiple_of((i - WARM) * BLOCK, BLOCK), BLOCK)
            c_ref[sl, :] = jnp.dot(a_loc[sl, :], b_full[col], preferred_element_type=jnp.float32)

        is_x = (i >= join) & (x_done < g_x) & ((x_done + 1) * GROUP <= i + 1)
        is_y = (i >= join) & (y_done < g_y) & ((y_done + 1) * GROUP + LAG <= i + 1)

        @pl.when(is_x)
        def _():
            remote(place(layer, x_done * GROUP, GROUP))

        @pl.when(is_y)
        def _():
            for k in range(GROUP):
                copy_y(1 - layer, y_done * GROUP + k).wait_recv()
            remote(place(1 - layer, y_done * GROUP, GROUP))

        return x_done + is_x.astype(jnp.int32), y_done + is_y.astype(jnp.int32)

    lax.fori_loop(0, max(n_x, g_y * GROUP + LAG), step, (0, 0))

    for k in range(g_y * GROUP, n_y):
        copy_y(1 - layer, k).wait_recv()
    if n_x % GROUP:
        remote(place(layer, g_x * GROUP, GROUP))

    lax.fori_loop(jnp.where(row == 0, START, 0), n_x, lambda i, u: (send_x(i).wait_send(), u)[1], 0)
    lax.fori_loop(0, n_y, lambda i, u: (copy_y(layer, i).wait_send(), u)[1], 0)
    swap_b(row).wait_send()


def solution(mesh):
    n_dep = mesh.shape['dep']

    def local_product(a_blk, b_blk):
        rows, depth = a_blk.shape
        width = b_blk.shape[1] // n_dep
        n_x = (rows // CHUNK + LEAD) // 2
        n_y = n_x - LEAD
        return pl.pallas_call(
            functools.partial(kernel, n_x, n_y),
            out_shape=pltpu.VMEM((rows, width), jnp.float32),
            in_specs=[pl.BlockSpec(memory_space=pltpu.HBM)] * 2,
            out_specs=pl.BlockSpec(memory_space=pltpu.VMEM),
            scratch_shapes=[
                pltpu.VMEM((rows, depth), jnp.bfloat16),
                pltpu.VMEM((rows, depth), jnp.bfloat16),
                pltpu.VMEM((2, depth, width), jnp.bfloat16),
                pltpu.SemaphoreType.DMA((HEAD + 2,)),
                pltpu.SemaphoreType.DMA,
                pltpu.SemaphoreType.DMA((n_x,)),
                pltpu.SemaphoreType.DMA((n_x,)),
                pltpu.SemaphoreType.DMA((n_y,)),
                pltpu.SemaphoreType.DMA((n_y,)),
                pltpu.SemaphoreType.DMA,
                pltpu.SemaphoreType.DMA,
                pltpu.SemaphoreType.REGULAR,
                pltpu.SemaphoreType.REGULAR,
                pltpu.SemaphoreType.REGULAR,
            ],
            compiler_params=pltpu.CompilerParams(collective_id=0, has_side_effects=True, vmem_limit_bytes=40 * 1024 * 1024),
            name='gather_dot',
        )(pltpu.with_memory_space_constraint(a_blk, pltpu.HBM), pltpu.with_memory_space_constraint(b_blk, pltpu.HBM))

    return jax.shard_map(local_product, mesh=mesh, in_specs=(P('row', 'col'), P('row', 'col')), out_specs=P('row', ('col', 'dep')), check_vma=False)
```

```python
import jax
import jax.numpy as jnp
from jax import lax
from jax.experimental import pallas as pl
from jax.experimental.pallas import tpu as pltpu
from jax.sharding import PartitionSpec as P

MESH = pl.DeviceIdType.MESH
CHUNK = 32
GROUP = 64 // CHUNK
TAKE = (25, 26)
LAG = 80 // CHUNK
HEAD = 64 // CHUNK
NEXT = 256 // CHUNK
BLOCK = 256
START = 0
WARM = 96 // CHUNK


def kernel(a_hbm, b_hbm, c_ref, a_loc, a_rem, b_full, a_sem, b_sem, x_send, x_recv, y_send, y_recv, d_send, d_recv, y_ready, d_ready, go):
    layer = lax.axis_index('dep')
    col = lax.axis_index('col')
    row = lax.axis_index('row')
    rows = a_loc.shape[0]
    width = b_full.shape[2]
    chunks = rows // CHUNK
    n_x = jnp.where(row == 0, TAKE[0], TAKE[1])
    n_y = chunks - n_x
    x_peer = (layer, 1 - col, row)
    y_peer = (1 - layer, col, row)
    d_peer = (layer, col, 1 - row)

    barrier = pltpu.get_barrier_semaphore()
    pl.semaphore_signal(barrier, inc=1, device_id=x_peer, device_id_type=MESH)

    @pl.when(layer == 0)
    def _():
        pl.semaphore_signal(barrier, inc=1, device_id=y_peer, device_id_type=MESH)

    @pl.when(row == 1)
    def _():
        pl.semaphore_signal(barrier, inc=1, device_id=d_peer, device_id_type=MESH)

    def place(owner, idx, count):
        start = idx * CHUNK + owner * (rows - (2 * idx + count) * CHUNK)
        return pl.ds(pl.multiple_of(start, CHUNK), count * CHUNK)

    def load_a(idx, count, sem):
        sl = place(layer, idx, count)
        return pltpu.make_async_copy(a_hbm.at[sl], a_loc.at[sl], a_sem.at[sem])

    loads = [load_a(i, 1, i) for i in range(HEAD)]
    loads.append(load_a(HEAD, NEXT - HEAD, HEAD))
    loads.append(load_a(NEXT, rows // CHUNK - NEXT, HEAD + 1))
    load_b = pltpu.make_async_copy(b_hbm.at[:, pl.ds(pl.multiple_of(layer * width, 128), width)], b_full.at[row], b_sem)

    def send_x(idx):
        sl = place(layer, idx, 1)
        return pltpu.make_async_remote_copy(
            src_ref=a_hbm.at[sl], dst_ref=a_rem.at[sl], send_sem=x_send.at[idx], recv_sem=x_recv.at[idx],
            device_id=x_peer, device_id_type=MESH)

    def copy_y(owner, idx):
        sl = place(owner, idx, 1)
        return pltpu.make_async_remote_copy(
            src_ref=a_rem.at[sl], dst_ref=a_rem.at[sl], send_sem=y_send.at[idx], recv_sem=y_recv.at[idx],
            device_id=y_peer, device_id_type=MESH)

    def swap_b(half):
        return pltpu.make_async_remote_copy(
            src_ref=b_full.at[half], dst_ref=b_full.at[half], send_sem=d_send, recv_sem=d_recv,
            device_id=d_peer, device_id_type=MESH)

    for copy in loads[:HEAD + 1]:
        copy.start()
    load_b.start()
    loads[HEAD + 1].start()

    pl.semaphore_wait(barrier, 2 + layer - row)

    def launch(i, u):
        send_x(i).start()
        return u

    @pl.when(row == 0)
    def _():
        lax.fori_loop(0, n_x, launch, 0)

    @pl.when(layer == 1)
    def _():
        pl.semaphore_signal(y_ready, inc=1, device_id=y_peer, device_id_type=MESH)

    @pl.when(row == 0)
    def _():
        pl.semaphore_signal(d_ready, inc=1, device_id=d_peer, device_id_type=MESH)

    load_b.wait()

    @pl.when(row == 1)
    def _():
        pl.semaphore_wait(d_ready, 1)

    swap_b(row).start()

    @pl.when(row == 0)
    def _():
        for i in range(START):
            send_x(i).wait_send()
        pl.semaphore_signal(go, inc=1, device_id=d_peer, device_id_type=MESH)

    for copy in loads:
        copy.wait()

    @pl.when(row == 1)
    def _():
        pl.semaphore_wait(go, 1)
        lax.fori_loop(0, n_x, launch, 0)

    @pl.when(layer == 0)
    def _():
        pl.semaphore_wait(y_ready, 1)

    def remote(sl):
        c_ref[sl, :] += jnp.dot(a_rem[sl, :], b_full[1 - col], preferred_element_type=jnp.float32)

    join = WARM + rows // BLOCK
    g_x = n_x // GROUP
    g_y = n_y // GROUP

    def step(i, done):
        x_done, y_done = done

        @pl.when(i < n_x)
        def _():
            send_x(i).wait_recv()

        @pl.when(i < n_y)
        def _():
            copy_y(layer, i).start()

        @pl.when(i == WARM)
        def _():
            swap_b(1 - row).wait_recv()

        @pl.when((i >= WARM) & (i < join))
        def _():
            sl = pl.ds(pl.multiple_of((i - WARM) * BLOCK, BLOCK), BLOCK)
            c_ref[sl, :] = jnp.dot(a_loc[sl, :], b_full[col], preferred_element_type=jnp.float32)

        is_x = (i >= join) & (x_done < g_x) & ((x_done + 1) * GROUP <= i + 1)
        is_y = (i >= join) & (y_done < g_y) & ((y_done + 1) * GROUP + LAG <= i + 1)

        @pl.when(is_x)
        def _():
            remote(place(layer, x_done * GROUP, GROUP))

        @pl.when(is_y)
        def _():
            for k in range(GROUP):
                copy_y(1 - layer, y_done * GROUP + k).wait_recv()
            remote(place(1 - layer, y_done * GROUP, GROUP))

        return x_done + is_x.astype(jnp.int32), y_done + is_y.astype(jnp.int32)

    lax.fori_loop(0, jnp.maximum(n_x, g_y * GROUP + LAG), step, (0, 0))

    lax.fori_loop(g_y * GROUP, n_y, lambda i, u: (copy_y(1 - layer, i).wait_recv(), u)[1], 0)

    @pl.when(g_x + g_y < chunks // GROUP)
    def _():
        remote(place(layer, g_x * GROUP, GROUP))

    lax.fori_loop(jnp.where(row == 0, START, 0), n_x, lambda i, u: (send_x(i).wait_send(), u)[1], 0)
    lax.fori_loop(0, n_y, lambda i, u: (copy_y(layer, i).wait_send(), u)[1], 0)
    swap_b(row).wait_send()


def solution(mesh):
    n_dep = mesh.shape['dep']

    def local_product(a_blk, b_blk):
        rows, depth = a_blk.shape
        width = b_blk.shape[1] // n_dep
        chunks = rows // CHUNK
        return pl.pallas_call(
            kernel,
            out_shape=pltpu.VMEM((rows, width), jnp.float32),
            in_specs=[pl.BlockSpec(memory_space=pltpu.HBM)] * 2,
            out_specs=pl.BlockSpec(memory_space=pltpu.VMEM),
            scratch_shapes=[
                pltpu.VMEM((rows, depth), jnp.bfloat16),
                pltpu.VMEM((rows, depth), jnp.bfloat16),
                pltpu.VMEM((2, depth, width), jnp.bfloat16),
                pltpu.SemaphoreType.DMA((HEAD + 2,)),
                pltpu.SemaphoreType.DMA,
                pltpu.SemaphoreType.DMA((chunks,)),
                pltpu.SemaphoreType.DMA((chunks,)),
                pltpu.SemaphoreType.DMA((chunks,)),
                pltpu.SemaphoreType.DMA((chunks,)),
                pltpu.SemaphoreType.DMA,
                pltpu.SemaphoreType.DMA,
                pltpu.SemaphoreType.REGULAR,
                pltpu.SemaphoreType.REGULAR,
                pltpu.SemaphoreType.REGULAR,
            ],
            compiler_params=pltpu.CompilerParams(collective_id=0, has_side_effects=True, vmem_limit_bytes=40 * 1024 * 1024),
            name='gather_dot',
        )(pltpu.with_memory_space_constraint(a_blk, pltpu.HBM), pltpu.with_memory_space_constraint(b_blk, pltpu.HBM))

    return jax.shard_map(local_product, mesh=mesh, in_specs=(P('row', 'col'), P('row', 'col')), out_specs=P('row', ('col', 'dep')), check_vma=False)
```

```python
import functools

import jax
import jax.numpy as jnp
from jax import lax
from jax.experimental import pallas as pl
from jax.experimental.pallas import tpu as pltpu
from jax.sharding import PartitionSpec as P

MESH = pl.DeviceIdType.MESH
CHUNK = 32
GROUP = 64 // CHUNK
LEAD = 64 // CHUNK
LAG = 80 // CHUNK
HEAD = 64 // CHUNK
NEXT = 256 // CHUNK
BLOCK = 256
WARM = 96 // CHUNK


def kernel(n_x, n_y, a_hbm, b_hbm, c_ref, a_rem, b_full, a_loc, a_sem, b_sem, x_send, x_recv, y_send, y_recv, d_send, d_recv, y_ready, d_ready):
    layer = lax.axis_index('dep')
    col = lax.axis_index('col')
    row = lax.axis_index('row')
    rows = a_loc.shape[0]
    width = b_full.shape[2]
    x_peer = (layer, 1 - col, row)
    y_peer = (1 - layer, col, row)
    d_peer = (layer, col, 1 - row)

    barrier = pltpu.get_barrier_semaphore()
    pl.semaphore_signal(barrier, inc=1, device_id=x_peer, device_id_type=MESH)

    @pl.when(layer == 0)
    def _():
        pl.semaphore_signal(barrier, inc=1, device_id=y_peer, device_id_type=MESH)

    @pl.when(row == 1)
    def _():
        pl.semaphore_signal(barrier, inc=1, device_id=d_peer, device_id_type=MESH)

    def place(owner, idx, count):
        start = idx * CHUNK + owner * (rows - (2 * idx + count) * CHUNK)
        return pl.ds(pl.multiple_of(start, CHUNK), count * CHUNK)

    def load_a(idx, count, sem):
        sl = place(layer, idx, count)
        return pltpu.make_async_copy(a_hbm.at[sl], a_loc.at[sl], a_sem.at[sem])

    loads = [load_a(i, 1, i) for i in range(HEAD)]
    loads.append(load_a(HEAD, NEXT - HEAD, HEAD))
    loads.append(load_a(NEXT, rows // CHUNK - NEXT, HEAD + 1))
    load_b = pltpu.make_async_copy(b_hbm.at[:, pl.ds(pl.multiple_of(layer * width, 128), width)], b_full.at[row], b_sem)

    def send_x(idx):
        sl = place(layer, idx, 1)
        return pltpu.make_async_remote_copy(
            src_ref=a_hbm.at[sl], dst_ref=a_rem.at[sl], send_sem=x_send.at[idx], recv_sem=x_recv.at[idx],
            device_id=x_peer, device_id_type=MESH)

    def copy_y(owner, idx):
        sl = place(owner, idx, 1)
        return pltpu.make_async_remote_copy(
            src_ref=a_rem.at[sl], dst_ref=a_rem.at[sl], send_sem=y_send.at[idx], recv_sem=y_recv.at[idx],
            device_id=y_peer, device_id_type=MESH)

    def swap_b(half):
        return pltpu.make_async_remote_copy(
            src_ref=b_full.at[half], dst_ref=b_full.at[half], send_sem=d_send, recv_sem=d_recv,
            device_id=d_peer, device_id_type=MESH)

    for copy in loads[:HEAD + 1]:
        copy.start()
    load_b.start()
    loads[HEAD + 1].start()

    pl.semaphore_wait(barrier, 2 + layer - row)

    for i in range(HEAD):
        send_x(i).start()

    @pl.when(layer == 1)
    def _():
        pl.semaphore_signal(y_ready, inc=1, device_id=y_peer, device_id_type=MESH)

    @pl.when(row == 0)
    def _():
        pl.semaphore_signal(d_ready, inc=1, device_id=d_peer, device_id_type=MESH)

    def launch(i, u):
        send_x(i).start()
        return u

    lax.fori_loop(HEAD, n_x, launch, 0)
    load_b.wait()

    @pl.when(row == 1)
    def _():
        pl.semaphore_wait(d_ready, 1)

    swap_b(row).start()
    for copy in loads:
        copy.wait()

    @pl.when(layer == 0)
    def _():
        pl.semaphore_wait(y_ready, 1)

    def remote(sl):
        c_ref[sl, :] += jnp.dot(a_rem[sl, :], b_full[1 - col], preferred_element_type=jnp.float32)

    join = WARM + rows // BLOCK
    g_x = n_x // GROUP
    g_y = n_y // GROUP

    def step(i, done):
        x_done, y_done = done

        @pl.when(i < n_x)
        def _():
            send_x(i).wait_recv()

        @pl.when(i < n_y)
        def _():
            copy_y(layer, i).start()

        @pl.when(i == WARM)
        def _():
            swap_b(1 - row).wait_recv()

        @pl.when((i >= WARM) & (i < join))
        def _():
            sl = pl.ds(pl.multiple_of((i - WARM) * BLOCK, BLOCK), BLOCK)
            c_ref[sl, :] = jnp.dot(a_loc[sl, :], b_full[col], preferred_element_type=jnp.float32)

        is_x = (i >= join) & (x_done < g_x) & ((x_done + 1) * GROUP <= i + 1)
        is_y = (i >= join) & (y_done < g_y) & ((y_done + 1) * GROUP + LAG <= i + 1)

        @pl.when(is_x)
        def _():
            remote(place(layer, x_done * GROUP, GROUP))

        @pl.when(is_y)
        def _():
            for k in range(GROUP):
                copy_y(1 - layer, y_done * GROUP + k).wait_recv()
            remote(place(1 - layer, y_done * GROUP, GROUP))

        return x_done + is_x.astype(jnp.int32), y_done + is_y.astype(jnp.int32)

    lax.fori_loop(0, max(n_x, g_y * GROUP + LAG), step, (0, 0))

    for k in range(g_y * GROUP, n_y):
        copy_y(1 - layer, k).wait_recv()
    lax.fori_loop(0, n_x, lambda i, u: (send_x(i).wait_send(), u)[1], 0)
    lax.fori_loop(0, n_y, lambda i, u: (copy_y(layer, i).wait_send(), u)[1], 0)
    swap_b(row).wait_send()


def finish(n_x, c_ref, a_rem, b_full, out, last, sem):
    layer = lax.axis_index('dep')
    col = lax.axis_index('col')
    rows = a_rem.shape[0]
    size = GROUP * CHUNK
    count = rows // size
    mine = n_x // GROUP + layer * (count - 1 - 2 * (n_x // GROUP))

    def block(i):
        return pl.ds(pl.multiple_of(i * size, size), size)

    def put(i):
        return pltpu.make_async_copy(c_ref.at[block(i)], out.at[block(i)], sem)

    def put_last():
        return pltpu.make_async_copy(last, out.at[block(mine)], sem)

    def start(i, u):
        @pl.when(i != mine)
        def _():
            put(i).start()

        return u

    lax.fori_loop(0, count, start, 0)
    last[...] = c_ref[block(mine), :] + jnp.dot(a_rem[block(mine), :], b_full[1 - col], preferred_element_type=jnp.float32)
    put_last().start()
    pltpu.make_async_copy(c_ref, out, sem).wait()


def solution(mesh):
    n_dep = mesh.shape['dep']

    def local_product(a_blk, b_blk):
        rows, depth = a_blk.shape
        width = b_blk.shape[1] // n_dep
        n_x = (rows // CHUNK + LEAD) // 2
        n_y = n_x - LEAD
        c, a_rem, b_full = pl.pallas_call(
            functools.partial(kernel, n_x, n_y),
            out_shape=(
                pltpu.VMEM((rows, width), jnp.float32),
                pltpu.VMEM((rows, depth), jnp.bfloat16),
                pltpu.VMEM((2, depth, width), jnp.bfloat16),
            ),
            in_specs=[pl.BlockSpec(memory_space=pltpu.HBM)] * 2,
            out_specs=(pl.BlockSpec(memory_space=pltpu.VMEM),) * 3,
            scratch_shapes=[
                pltpu.VMEM((rows, depth), jnp.bfloat16),
                pltpu.SemaphoreType.DMA((HEAD + 2,)),
                pltpu.SemaphoreType.DMA,
                pltpu.SemaphoreType.DMA((n_x,)),
                pltpu.SemaphoreType.DMA((n_x,)),
                pltpu.SemaphoreType.DMA((n_y,)),
                pltpu.SemaphoreType.DMA((n_y,)),
                pltpu.SemaphoreType.DMA,
                pltpu.SemaphoreType.DMA,
                pltpu.SemaphoreType.REGULAR,
                pltpu.SemaphoreType.REGULAR,
            ],
            compiler_params=pltpu.CompilerParams(collective_id=0, has_side_effects=True, vmem_limit_bytes=40 * 1024 * 1024),
            name='gather_dot',
        )(pltpu.with_memory_space_constraint(a_blk, pltpu.HBM), pltpu.with_memory_space_constraint(b_blk, pltpu.HBM))

        return pl.pallas_call(
            functools.partial(finish, n_x),
            out_shape=pltpu.HBM((rows, width), jnp.float32),
            in_specs=[pl.BlockSpec(memory_space=pltpu.VMEM)] * 3,
            out_specs=pl.BlockSpec(memory_space=pltpu.HBM),
            scratch_shapes=[pltpu.VMEM((GROUP * CHUNK, width), jnp.float32), pltpu.SemaphoreType.DMA],
            compiler_params=pltpu.CompilerParams(vmem_limit_bytes=8 * 1024 * 1024),
            name='finish',
        )(*(pltpu.with_memory_space_constraint(v, pltpu.VMEM) for v in (c, a_rem, b_full)))

    return jax.shard_map(local_product, mesh=mesh, in_specs=(P('row', 'col'), P('row', 'col')), out_specs=P('row', ('col', 'dep')), check_vma=False)
```

```python
import functools

import jax
import jax.numpy as jnp
from jax import lax
from jax.experimental import pallas as pl
from jax.experimental.pallas import tpu as pltpu
from jax.sharding import PartitionSpec as P

MESH = pl.DeviceIdType.MESH
CHUNK = 32
GROUP = 64 // CHUNK
LEAD = 96 // CHUNK
HALF = CHUNK // 2
LAG = 80 // CHUNK
HEAD = 64 // CHUNK
NEXT = 256 // CHUNK
BLOCK = 256
WARM = 96 // CHUNK


def kernel(n_x, n_y, a_hbm, b_hbm, c_ref, a_rem, b_full, a_loc, a_sem, b_sem, x_send, x_recv, y_send, y_recv, d_send, d_recv, y_ready, d_ready):
    layer = lax.axis_index('dep')
    col = lax.axis_index('col')
    row = lax.axis_index('row')
    rows = a_loc.shape[0]
    width = b_full.shape[2]
    x_peer = (layer, 1 - col, row)
    y_peer = (1 - layer, col, row)
    d_peer = (layer, col, 1 - row)

    barrier = pltpu.get_barrier_semaphore()
    pl.semaphore_signal(barrier, inc=1, device_id=x_peer, device_id_type=MESH)

    @pl.when(layer == 0)
    def _():
        pl.semaphore_signal(barrier, inc=1, device_id=y_peer, device_id_type=MESH)

    @pl.when(row == 1)
    def _():
        pl.semaphore_signal(barrier, inc=1, device_id=d_peer, device_id_type=MESH)

    def place(owner, idx, count):
        start = idx * CHUNK + owner * (rows - (2 * idx + count) * CHUNK)
        return pl.ds(pl.multiple_of(start, CHUNK), count * CHUNK)

    def half(owner, idx):
        start = idx * CHUNK
        return pl.ds(pl.multiple_of(start + owner * (rows - 2 * start - HALF), HALF), HALF)

    def load_a(idx, count, sem):
        sl = place(layer, idx, count)
        return pltpu.make_async_copy(a_hbm.at[sl], a_loc.at[sl], a_sem.at[sem])

    loads = [load_a(i, 1, i) for i in range(HEAD)]
    loads.append(load_a(HEAD, NEXT - HEAD, HEAD))
    loads.append(load_a(NEXT, rows // CHUNK - NEXT, HEAD + 1))
    load_b = pltpu.make_async_copy(b_hbm.at[:, pl.ds(pl.multiple_of(layer * width, 128), width)], b_full.at[row], b_sem)

    def send_x(idx):
        sl = place(layer, idx, 1)
        return pltpu.make_async_remote_copy(
            src_ref=a_hbm.at[sl], dst_ref=a_rem.at[sl], send_sem=x_send.at[idx], recv_sem=x_recv.at[idx],
            device_id=x_peer, device_id_type=MESH)

    def copy_y(owner, idx):
        sl = place(owner, idx, 1)
        return pltpu.make_async_remote_copy(
            src_ref=a_rem.at[sl], dst_ref=a_rem.at[sl], send_sem=y_send.at[idx], recv_sem=y_recv.at[idx],
            device_id=y_peer, device_id_type=MESH)

    half_x = pltpu.make_async_remote_copy(
        src_ref=a_hbm.at[half(layer, n_x)], dst_ref=a_rem.at[half(layer, n_x)], send_sem=x_send.at[n_x], recv_sem=x_recv.at[n_x],
        device_id=x_peer, device_id_type=MESH)

    def half_y(owner):
        sl = half(owner, n_y)
        return pltpu.make_async_remote_copy(
            src_ref=a_rem.at[sl], dst_ref=a_rem.at[sl], send_sem=y_send.at[n_y], recv_sem=y_recv.at[n_y],
            device_id=y_peer, device_id_type=MESH)

    def swap_b(side):
        return pltpu.make_async_remote_copy(
            src_ref=b_full.at[side], dst_ref=b_full.at[side], send_sem=d_send, recv_sem=d_recv,
            device_id=d_peer, device_id_type=MESH)

    for copy in loads[:HEAD + 1]:
        copy.start()
    load_b.start()
    loads[HEAD + 1].start()

    pl.semaphore_wait(barrier, 2 + layer - row)

    for i in range(HEAD):
        send_x(i).start()

    @pl.when(layer == 1)
    def _():
        pl.semaphore_signal(y_ready, inc=1, device_id=y_peer, device_id_type=MESH)

    @pl.when(row == 0)
    def _():
        pl.semaphore_signal(d_ready, inc=1, device_id=d_peer, device_id_type=MESH)

    def launch(i, u):
        send_x(i).start()
        return u

    lax.fori_loop(HEAD, n_x, launch, 0)
    half_x.start()
    load_b.wait()

    @pl.when(row == 1)
    def _():
        pl.semaphore_wait(d_ready, 1)

    swap_b(row).start()
    for copy in loads:
        copy.wait()

    @pl.when(layer == 0)
    def _():
        pl.semaphore_wait(y_ready, 1)

    def remote(sl):
        c_ref[sl, :] += jnp.dot(a_rem[sl, :], b_full[1 - col], preferred_element_type=jnp.float32)

    join = WARM + rows // BLOCK
    g_x = n_x // GROUP
    g_y = n_y // GROUP

    def step(i, done):
        x_done, y_done = done

        @pl.when(i < n_x)
        def _():
            send_x(i).wait_recv()

        @pl.when(i < n_y)
        def _():
            copy_y(layer, i).start()

        @pl.when(i == n_y)
        def _():
            half_y(layer).start()

        @pl.when(i == WARM)
        def _():
            swap_b(1 - row).wait_recv()

        @pl.when((i >= WARM) & (i < join))
        def _():
            sl = pl.ds(pl.multiple_of((i - WARM) * BLOCK, BLOCK), BLOCK)
            c_ref[sl, :] = jnp.dot(a_loc[sl, :], b_full[col], preferred_element_type=jnp.float32)

        is_x = (i >= join) & (x_done < g_x) & ((x_done + 1) * GROUP <= i + 1)
        is_y = (i >= join) & (y_done < g_y) & ((y_done + 1) * GROUP + LAG <= i + 1)

        @pl.when(is_x)
        def _():
            remote(place(layer, x_done * GROUP, GROUP))

        @pl.when(is_y)
        def _():
            for k in range(GROUP):
                copy_y(1 - layer, y_done * GROUP + k).wait_recv()
            remote(place(1 - layer, y_done * GROUP, GROUP))

        return x_done + is_x.astype(jnp.int32), y_done + is_y.astype(jnp.int32)

    lax.fori_loop(0, max(n_x, g_y * GROUP + LAG), step, (0, 0))

    for k in range(g_y * GROUP, n_y):
        copy_y(1 - layer, k).wait_recv()
    half_x.wait_recv()
    half_y(1 - layer).wait_recv()

    lax.fori_loop(0, n_x, lambda i, u: (send_x(i).wait_send(), u)[1], 0)
    lax.fori_loop(0, n_y, lambda i, u: (copy_y(layer, i).wait_send(), u)[1], 0)
    half_x.wait_send()
    half_y(layer).wait_send()
    swap_b(row).wait_send()


def finish(n_x, c_ref, a_rem, b_full, out, last, sem):
    layer = lax.axis_index('dep')
    col = lax.axis_index('col')
    rows = a_rem.shape[0]
    size = GROUP * CHUNK
    count = rows // size
    mine = n_x // GROUP + layer * (count - 1 - 2 * (n_x // GROUP))

    def block(i):
        return pl.ds(pl.multiple_of(i * size, size), size)

    def put(i):
        return pltpu.make_async_copy(c_ref.at[block(i)], out.at[block(i)], sem)

    def put_last():
        return pltpu.make_async_copy(last, out.at[block(mine)], sem)

    def start(i, u):
        @pl.when(i != mine)
        def _():
            put(i).start()

        return u

    lax.fori_loop(0, count, start, 0)
    last[...] = c_ref[block(mine), :] + jnp.dot(a_rem[block(mine), :], b_full[1 - col], preferred_element_type=jnp.float32)
    put_last().start()
    pltpu.make_async_copy(c_ref, out, sem).wait()


def solution(mesh):
    n_dep = mesh.shape['dep']

    def local_product(a_blk, b_blk):
        rows, depth = a_blk.shape
        width = b_blk.shape[1] // n_dep
        n_x = (rows // CHUNK + LEAD - 1) // 2
        n_y = n_x - LEAD
        c, a_rem, b_full = pl.pallas_call(
            functools.partial(kernel, n_x, n_y),
            out_shape=(
                pltpu.VMEM((rows, width), jnp.float32),
                pltpu.VMEM((rows, depth), jnp.bfloat16),
                pltpu.VMEM((2, depth, width), jnp.bfloat16),
            ),
            in_specs=[pl.BlockSpec(memory_space=pltpu.HBM)] * 2,
            out_specs=(pl.BlockSpec(memory_space=pltpu.VMEM),) * 3,
            scratch_shapes=[
                pltpu.VMEM((rows, depth), jnp.bfloat16),
                pltpu.SemaphoreType.DMA((HEAD + 2,)),
                pltpu.SemaphoreType.DMA,
                pltpu.SemaphoreType.DMA((n_x + 1,)),
                pltpu.SemaphoreType.DMA((n_x + 1,)),
                pltpu.SemaphoreType.DMA((n_y + 1,)),
                pltpu.SemaphoreType.DMA((n_y + 1,)),
                pltpu.SemaphoreType.DMA,
                pltpu.SemaphoreType.DMA,
                pltpu.SemaphoreType.REGULAR,
                pltpu.SemaphoreType.REGULAR,
            ],
            compiler_params=pltpu.CompilerParams(collective_id=0, has_side_effects=True, vmem_limit_bytes=40 * 1024 * 1024),
            name='gather_dot',
        )(pltpu.with_memory_space_constraint(a_blk, pltpu.HBM), pltpu.with_memory_space_constraint(b_blk, pltpu.HBM))

        return pl.pallas_call(
            functools.partial(finish, n_x),
            out_shape=pltpu.HBM((rows, width), jnp.float32),
            in_specs=[pl.BlockSpec(memory_space=pltpu.VMEM)] * 3,
            out_specs=pl.BlockSpec(memory_space=pltpu.HBM),
            scratch_shapes=[pltpu.VMEM((GROUP * CHUNK, width), jnp.float32), pltpu.SemaphoreType.DMA],
            compiler_params=pltpu.CompilerParams(vmem_limit_bytes=8 * 1024 * 1024),
            name='finish',
        )(*(pltpu.with_memory_space_constraint(v, pltpu.VMEM) for v in (c, a_rem, b_full)))

    return jax.shard_map(local_product, mesh=mesh, in_specs=(P('row', 'col'), P('row', 'col')), out_specs=P('row', ('col', 'dep')), check_vma=False)
```

```python
import functools

import jax
import jax.numpy as jnp
from jax import lax
from jax.experimental import pallas as pl
from jax.experimental.pallas import tpu as pltpu
from jax.sharding import PartitionSpec as P

MESH = pl.DeviceIdType.MESH
CHUNK = 32
GROUP = 64 // CHUNK
LEAD = 96 // CHUNK
HALF = CHUNK // 2
LAG = 80 // CHUNK
HEAD = 64 // CHUNK
NEXT = 256 // CHUNK
BLOCK = 256
HOLD = 21
WARM = 96 // CHUNK


def kernel(n_x, n_y, a_hbm, b_hbm, c_ref, a_rem, b_full, a_loc, a_sem, b_sem, x_send, x_recv, y_send, y_recv, d_send, d_recv, y_ready, d_ready):
    layer = lax.axis_index('dep')
    col = lax.axis_index('col')
    row = lax.axis_index('row')
    rows = a_loc.shape[0]
    width = b_full.shape[2]
    x_peer = (layer, 1 - col, row)
    y_peer = (1 - layer, col, row)
    d_peer = (layer, col, 1 - row)

    barrier = pltpu.get_barrier_semaphore()
    pl.semaphore_signal(barrier, inc=1, device_id=x_peer, device_id_type=MESH)

    @pl.when(layer == 0)
    def _():
        pl.semaphore_signal(barrier, inc=1, device_id=y_peer, device_id_type=MESH)

    @pl.when(row == 1)
    def _():
        pl.semaphore_signal(barrier, inc=1, device_id=d_peer, device_id_type=MESH)

    def place(owner, idx, count):
        start = idx * CHUNK + owner * (rows - (2 * idx + count) * CHUNK)
        return pl.ds(pl.multiple_of(start, CHUNK), count * CHUNK)

    def half(owner, idx):
        start = idx * CHUNK
        return pl.ds(pl.multiple_of(start + owner * (rows - 2 * start - HALF), HALF), HALF)

    def load_a(idx, count, sem):
        sl = place(layer, idx, count)
        return pltpu.make_async_copy(a_hbm.at[sl], a_loc.at[sl], a_sem.at[sem])

    loads = [load_a(i, 1, i) for i in range(HEAD)]
    loads.append(load_a(HEAD, NEXT - HEAD, HEAD))
    loads.append(load_a(NEXT, rows // CHUNK - NEXT, HEAD + 1))
    load_b = pltpu.make_async_copy(b_hbm.at[:, pl.ds(pl.multiple_of(layer * width, 128), width)], b_full.at[row], b_sem)

    def send_x(idx):
        sl = place(layer, idx, 1)
        return pltpu.make_async_remote_copy(
            src_ref=a_hbm.at[sl], dst_ref=a_rem.at[sl], send_sem=x_send.at[idx], recv_sem=x_recv.at[idx],
            device_id=x_peer, device_id_type=MESH)

    def copy_y(owner, idx):
        sl = place(owner, idx, 1)
        return pltpu.make_async_remote_copy(
            src_ref=a_rem.at[sl], dst_ref=a_rem.at[sl], send_sem=y_send.at[idx], recv_sem=y_recv.at[idx],
            device_id=y_peer, device_id_type=MESH)

    half_x = pltpu.make_async_remote_copy(
        src_ref=a_hbm.at[half(layer, n_x)], dst_ref=a_rem.at[half(layer, n_x)], send_sem=x_send.at[n_x], recv_sem=x_recv.at[n_x],
        device_id=x_peer, device_id_type=MESH)

    def half_y(owner):
        sl = half(owner, n_y)
        return pltpu.make_async_remote_copy(
            src_ref=a_rem.at[sl], dst_ref=a_rem.at[sl], send_sem=y_send.at[n_y], recv_sem=y_recv.at[n_y],
            device_id=y_peer, device_id_type=MESH)

    def swap_b(side):
        return pltpu.make_async_remote_copy(
            src_ref=b_full.at[side], dst_ref=b_full.at[side], send_sem=d_send, recv_sem=d_recv,
            device_id=d_peer, device_id_type=MESH)

    for copy in loads[:HEAD + 1]:
        copy.start()
    load_b.start()
    loads[HEAD + 1].start()

    pl.semaphore_wait(barrier, 2 + layer - row)

    for i in range(HEAD):
        send_x(i).start()

    @pl.when(layer == 1)
    def _():
        pl.semaphore_signal(y_ready, inc=1, device_id=y_peer, device_id_type=MESH)

    @pl.when(row == 0)
    def _():
        pl.semaphore_signal(d_ready, inc=1, device_id=d_peer, device_id_type=MESH)

    def launch(i, u):
        send_x(i).start()
        return u

    first_out = jnp.where(row == 0, n_x, HOLD)
    lax.fori_loop(HEAD, first_out, launch, 0)

    @pl.when(row == 0)
    def _():
        half_x.start()

    load_b.wait()

    @pl.when(row == 1)
    def _():
        pl.semaphore_wait(d_ready, 1)

    swap_b(row).start()
    for copy in loads:
        copy.wait()

    @pl.when(layer == 0)
    def _():
        pl.semaphore_wait(y_ready, 1)

    def remote(sl):
        c_ref[sl, :] += jnp.dot(a_rem[sl, :], b_full[1 - col], preferred_element_type=jnp.float32)

    join = WARM + rows // BLOCK
    g_x = n_x // GROUP
    g_y = n_y // GROUP

    def step(i, done):
        x_done, y_done = done

        @pl.when(i < n_x)
        def _():
            send_x(i).wait_recv()

        @pl.when(i < n_y)
        def _():
            copy_y(layer, i).start()

        @pl.when(i == n_y)
        def _():
            half_y(layer).start()

        @pl.when((i == HOLD - 1) & (row == 1))
        def _():
            lax.fori_loop(first_out, n_x, launch, 0)
            half_x.start()

        @pl.when(i == WARM)
        def _():
            swap_b(1 - row).wait_recv()

        @pl.when((i >= WARM) & (i < join))
        def _():
            sl = pl.ds(pl.multiple_of((i - WARM) * BLOCK, BLOCK), BLOCK)
            c_ref[sl, :] = jnp.dot(a_loc[sl, :], b_full[col], preferred_element_type=jnp.float32)

        is_x = (i >= join) & (x_done < g_x) & ((x_done + 1) * GROUP <= i + 1)
        is_y = (i >= join) & (y_done < g_y) & ((y_done + 1) * GROUP + LAG <= i + 1)

        @pl.when(is_x)
        def _():
            remote(place(layer, x_done * GROUP, GROUP))

        @pl.when(is_y)
        def _():
            for k in range(GROUP):
                copy_y(1 - layer, y_done * GROUP + k).wait_recv()
            remote(place(1 - layer, y_done * GROUP, GROUP))

        return x_done + is_x.astype(jnp.int32), y_done + is_y.astype(jnp.int32)

    lax.fori_loop(0, max(n_x, g_y * GROUP + LAG), step, (0, 0))

    for k in range(g_y * GROUP, n_y):
        copy_y(1 - layer, k).wait_recv()
    half_x.wait_recv()
    half_y(1 - layer).wait_recv()

    lax.fori_loop(0, n_x, lambda i, u: (send_x(i).wait_send(), u)[1], 0)
    lax.fori_loop(0, n_y, lambda i, u: (copy_y(layer, i).wait_send(), u)[1], 0)
    half_x.wait_send()
    half_y(layer).wait_send()
    swap_b(row).wait_send()


def finish(n_x, c_ref, a_rem, b_full, out, last, sem):
    layer = lax.axis_index('dep')
    col = lax.axis_index('col')
    rows = a_rem.shape[0]
    size = GROUP * CHUNK
    count = rows // size
    mine = n_x // GROUP + layer * (count - 1 - 2 * (n_x // GROUP))

    def block(i):
        return pl.ds(pl.multiple_of(i * size, size), size)

    def put(i):
        return pltpu.make_async_copy(c_ref.at[block(i)], out.at[block(i)], sem)

    def put_last():
        return pltpu.make_async_copy(last, out.at[block(mine)], sem)

    def start(i, u):
        @pl.when(i != mine)
        def _():
            put(i).start()

        return u

    lax.fori_loop(0, count, start, 0)
    last[...] = c_ref[block(mine), :] + jnp.dot(a_rem[block(mine), :], b_full[1 - col], preferred_element_type=jnp.float32)
    put_last().start()
    pltpu.make_async_copy(c_ref, out, sem).wait()


def solution(mesh):
    n_dep = mesh.shape['dep']

    def local_product(a_blk, b_blk):
        rows, depth = a_blk.shape
        width = b_blk.shape[1] // n_dep
        n_x = (rows // CHUNK + LEAD - 1) // 2
        n_y = n_x - LEAD
        c, a_rem, b_full = pl.pallas_call(
            functools.partial(kernel, n_x, n_y),
            out_shape=(
                pltpu.VMEM((rows, width), jnp.float32),
                pltpu.VMEM((rows, depth), jnp.bfloat16),
                pltpu.VMEM((2, depth, width), jnp.bfloat16),
            ),
            in_specs=[pl.BlockSpec(memory_space=pltpu.HBM)] * 2,
            out_specs=(pl.BlockSpec(memory_space=pltpu.VMEM),) * 3,
            scratch_shapes=[
                pltpu.VMEM((rows, depth), jnp.bfloat16),
                pltpu.SemaphoreType.DMA((HEAD + 2,)),
                pltpu.SemaphoreType.DMA,
                pltpu.SemaphoreType.DMA((n_x + 1,)),
                pltpu.SemaphoreType.DMA((n_x + 1,)),
                pltpu.SemaphoreType.DMA((n_y + 1,)),
                pltpu.SemaphoreType.DMA((n_y + 1,)),
                pltpu.SemaphoreType.DMA,
                pltpu.SemaphoreType.DMA,
                pltpu.SemaphoreType.REGULAR,
                pltpu.SemaphoreType.REGULAR,
            ],
            compiler_params=pltpu.CompilerParams(collective_id=0, has_side_effects=True, vmem_limit_bytes=40 * 1024 * 1024),
            name='gather_dot',
        )(pltpu.with_memory_space_constraint(a_blk, pltpu.HBM), pltpu.with_memory_space_constraint(b_blk, pltpu.HBM))

        return pl.pallas_call(
            functools.partial(finish, n_x),
            out_shape=pltpu.HBM((rows, width), jnp.float32),
            in_specs=[pl.BlockSpec(memory_space=pltpu.VMEM)] * 3,
            out_specs=pl.BlockSpec(memory_space=pltpu.HBM),
            scratch_shapes=[pltpu.VMEM((GROUP * CHUNK, width), jnp.float32), pltpu.SemaphoreType.DMA],
            compiler_params=pltpu.CompilerParams(vmem_limit_bytes=8 * 1024 * 1024),
            name='finish',
        )(*(pltpu.with_memory_space_constraint(v, pltpu.VMEM) for v in (c, a_rem, b_full)))

    return jax.shard_map(local_product, mesh=mesh, in_specs=(P('row', 'col'), P('row', 'col')), out_specs=P('row', ('col', 'dep')), check_vma=False)
```

```python
import functools

import jax
import jax.numpy as jnp
from jax import lax
from jax.experimental import pallas as pl
from jax.experimental.pallas import tpu as pltpu
from jax.sharding import PartitionSpec as P

MESH = pl.DeviceIdType.MESH
CHUNK = 32
GROUP = 64 // CHUNK
LEAD = 96 // CHUNK
HALF = CHUNK // 2
LAG = 80 // CHUNK
HEAD = 64 // CHUNK
NEXT = 256 // CHUNK
BLOCK = 256
HOLD = 21
WARM = 96 // CHUNK


def kernel(n_x, n_y, a_hbm, b_hbm, c_ref, a_rem, b_full, a_loc, a_sem, b_sem, x_send, x_recv, y_send, y_recv, d_send, d_recv, y_ready, d_ready):
    layer = lax.axis_index('dep')
    col = lax.axis_index('col')
    row = lax.axis_index('row')
    rows = a_loc.shape[0]
    width = b_full.shape[2]
    x_peer = (layer, 1 - col, row)
    y_peer = (1 - layer, col, row)
    d_peer = (layer, col, 1 - row)

    barrier = pltpu.get_barrier_semaphore()
    pl.semaphore_signal(barrier, inc=1, device_id=x_peer, device_id_type=MESH)

    @pl.when(layer == 0)
    def _():
        pl.semaphore_signal(barrier, inc=1, device_id=y_peer, device_id_type=MESH)

    @pl.when(row == 1)
    def _():
        pl.semaphore_signal(barrier, inc=1, device_id=d_peer, device_id_type=MESH)

    def place(owner, idx, count):
        start = idx * CHUNK + owner * (rows - (2 * idx + count) * CHUNK)
        return pl.ds(pl.multiple_of(start, CHUNK), count * CHUNK)

    def half(owner, idx):
        start = idx * CHUNK
        return pl.ds(pl.multiple_of(start + owner * (rows - 2 * start - HALF), HALF), HALF)

    def load_a(idx, count, sem):
        sl = place(layer, idx, count)
        return pltpu.make_async_copy(a_hbm.at[sl], a_loc.at[sl], a_sem.at[sem])

    loads = [load_a(i, 1, i) for i in range(HEAD)]
    loads.append(load_a(HEAD, NEXT - HEAD, HEAD))
    loads.append(load_a(NEXT, rows // CHUNK - NEXT, HEAD + 1))
    load_b = pltpu.make_async_copy(b_hbm.at[:, pl.ds(pl.multiple_of(layer * width, 128), width)], b_full.at[row], b_sem)

    def send_x(idx):
        sl = place(layer, idx, 1)
        return pltpu.make_async_remote_copy(
            src_ref=a_hbm.at[sl], dst_ref=a_rem.at[sl], send_sem=x_send.at[idx], recv_sem=x_recv.at[idx],
            device_id=x_peer, device_id_type=MESH)

    def copy_y(owner, idx):
        sl = place(owner, idx, 1)
        return pltpu.make_async_remote_copy(
            src_ref=a_rem.at[sl], dst_ref=a_rem.at[sl], send_sem=y_send.at[idx], recv_sem=y_recv.at[idx],
            device_id=y_peer, device_id_type=MESH)

    half_x = pltpu.make_async_remote_copy(
        src_ref=a_hbm.at[half(layer, n_x)], dst_ref=a_rem.at[half(layer, n_x)], send_sem=x_send.at[n_x], recv_sem=x_recv.at[n_x],
        device_id=x_peer, device_id_type=MESH)

    def half_y(owner):
        sl = half(owner, n_y)
        return pltpu.make_async_remote_copy(
            src_ref=a_rem.at[sl], dst_ref=a_rem.at[sl], send_sem=y_send.at[n_y], recv_sem=y_recv.at[n_y],
            device_id=y_peer, device_id_type=MESH)

    def swap_b(side):
        return pltpu.make_async_remote_copy(
            src_ref=b_full.at[side], dst_ref=b_full.at[side], send_sem=d_send, recv_sem=d_recv,
            device_id=d_peer, device_id_type=MESH)

    for copy in loads[:HEAD + 1]:
        copy.start()
    load_b.start()
    loads[HEAD + 1].start()

    pl.semaphore_wait(barrier, 2 + layer - row)

    for i in range(HEAD):
        send_x(i).start()

    @pl.when(layer == 1)
    def _():
        pl.semaphore_signal(y_ready, inc=1, device_id=y_peer, device_id_type=MESH)

    @pl.when(row == 0)
    def _():
        pl.semaphore_signal(d_ready, inc=1, device_id=d_peer, device_id_type=MESH)

    def launch(i, u):
        send_x(i).start()
        return u

    first_out = jnp.where(row == 0, n_x, HOLD)
    lax.fori_loop(HEAD, first_out, launch, 0)

    @pl.when(row == 0)
    def _():
        half_x.start()

    load_b.wait()

    @pl.when(row == 1)
    def _():
        pl.semaphore_wait(d_ready, 1)

    swap_b(row).start()
    for copy in loads:
        copy.wait()

    @pl.when(layer == 0)
    def _():
        pl.semaphore_wait(y_ready, 1)

    def remote(sl):
        c_ref[sl, :] += jnp.dot(a_rem[sl, :], b_full[1 - col], preferred_element_type=jnp.float32)

    join = WARM + rows // BLOCK
    g_x = n_x // GROUP
    g_y = n_y // GROUP

    def step(i, done):
        x_done, y_done = done

        @pl.when(i < n_x)
        def _():
            send_x(i).wait_recv()

        @pl.when(i < n_y)
        def _():
            copy_y(layer, i).start()

        @pl.when((i == n_y) & (row == 0))
        def _():
            half_y(layer).start()

        @pl.when((i == n_y) & (row == 1))
        def _():
            copy_y(layer, n_y).start()

        @pl.when((i == HOLD - 1) & (row == 1))
        def _():
            lax.fori_loop(first_out, n_x, launch, 0)

        @pl.when(i == WARM)
        def _():
            swap_b(1 - row).wait_recv()

        @pl.when((i >= WARM) & (i < join))
        def _():
            sl = pl.ds(pl.multiple_of((i - WARM) * BLOCK, BLOCK), BLOCK)
            c_ref[sl, :] = jnp.dot(a_loc[sl, :], b_full[col], preferred_element_type=jnp.float32)

        is_x = (i >= join) & (x_done < g_x) & ((x_done + 1) * GROUP <= i + 1)
        is_y = (i >= join) & (y_done < g_y) & ((y_done + 1) * GROUP + LAG <= i + 1)

        @pl.when(is_x)
        def _():
            remote(place(layer, x_done * GROUP, GROUP))

        @pl.when(is_y)
        def _():
            for k in range(GROUP):
                copy_y(1 - layer, y_done * GROUP + k).wait_recv()
            remote(place(1 - layer, y_done * GROUP, GROUP))

        return x_done + is_x.astype(jnp.int32), y_done + is_y.astype(jnp.int32)

    lax.fori_loop(0, max(n_x, g_y * GROUP + LAG), step, (0, 0))

    for k in range(g_y * GROUP, n_y):
        copy_y(1 - layer, k).wait_recv()
    @pl.when(row == 0)
    def _():
        half_x.wait_recv()
        half_y(1 - layer).wait_recv()

    @pl.when(row == 1)
    def _():
        copy_y(1 - layer, n_y).wait_recv()

    lax.fori_loop(0, n_x, lambda i, u: (send_x(i).wait_send(), u)[1], 0)
    lax.fori_loop(0, n_y, lambda i, u: (copy_y(layer, i).wait_send(), u)[1], 0)

    @pl.when(row == 0)
    def _():
        half_x.wait_send()
        half_y(layer).wait_send()

    @pl.when(row == 1)
    def _():
        copy_y(layer, n_y).wait_send()

    swap_b(row).wait_send()


def finish(n_x, c_ref, a_rem, b_full, out, last, sem):
    layer = lax.axis_index('dep')
    col = lax.axis_index('col')
    rows = a_rem.shape[0]
    size = GROUP * CHUNK
    count = rows // size
    mine = n_x // GROUP + layer * (count - 1 - 2 * (n_x // GROUP))

    def block(i):
        return pl.ds(pl.multiple_of(i * size, size), size)

    def put(i):
        return pltpu.make_async_copy(c_ref.at[block(i)], out.at[block(i)], sem)

    def put_last():
        return pltpu.make_async_copy(last, out.at[block(mine)], sem)

    def start(i, u):
        @pl.when(i != mine)
        def _():
            put(i).start()

        return u

    lax.fori_loop(0, count, start, 0)
    last[...] = c_ref[block(mine), :] + jnp.dot(a_rem[block(mine), :], b_full[1 - col], preferred_element_type=jnp.float32)
    put_last().start()
    pltpu.make_async_copy(c_ref, out, sem).wait()


def solution(mesh):
    n_dep = mesh.shape['dep']

    def local_product(a_blk, b_blk):
        rows, depth = a_blk.shape
        width = b_blk.shape[1] // n_dep
        n_x = (rows // CHUNK + LEAD - 1) // 2
        n_y = n_x - LEAD
        c, a_rem, b_full = pl.pallas_call(
            functools.partial(kernel, n_x, n_y),
            out_shape=(
                pltpu.VMEM((rows, width), jnp.float32),
                pltpu.VMEM((rows, depth), jnp.bfloat16),
                pltpu.VMEM((2, depth, width), jnp.bfloat16),
            ),
            in_specs=[pl.BlockSpec(memory_space=pltpu.HBM)] * 2,
            out_specs=(pl.BlockSpec(memory_space=pltpu.VMEM),) * 3,
            scratch_shapes=[
                pltpu.VMEM((rows, depth), jnp.bfloat16),
                pltpu.SemaphoreType.DMA((HEAD + 2,)),
                pltpu.SemaphoreType.DMA,
                pltpu.SemaphoreType.DMA((n_x + 1,)),
                pltpu.SemaphoreType.DMA((n_x + 1,)),
                pltpu.SemaphoreType.DMA((n_y + 1,)),
                pltpu.SemaphoreType.DMA((n_y + 1,)),
                pltpu.SemaphoreType.DMA,
                pltpu.SemaphoreType.DMA,
                pltpu.SemaphoreType.REGULAR,
                pltpu.SemaphoreType.REGULAR,
            ],
            compiler_params=pltpu.CompilerParams(collective_id=0, has_side_effects=True, vmem_limit_bytes=40 * 1024 * 1024),
            name='gather_dot',
        )(pltpu.with_memory_space_constraint(a_blk, pltpu.HBM), pltpu.with_memory_space_constraint(b_blk, pltpu.HBM))

        return pl.pallas_call(
            functools.partial(finish, n_x),
            out_shape=pltpu.HBM((rows, width), jnp.float32),
            in_specs=[pl.BlockSpec(memory_space=pltpu.VMEM)] * 3,
            out_specs=pl.BlockSpec(memory_space=pltpu.HBM),
            scratch_shapes=[pltpu.VMEM((GROUP * CHUNK, width), jnp.float32), pltpu.SemaphoreType.DMA],
            compiler_params=pltpu.CompilerParams(vmem_limit_bytes=8 * 1024 * 1024),
            name='finish',
        )(*(pltpu.with_memory_space_constraint(v, pltpu.VMEM) for v in (c, a_rem, b_full)))

    return jax.shard_map(local_product, mesh=mesh, in_specs=(P('row', 'col'), P('row', 'col')), out_specs=P('row', ('col', 'dep')), check_vma=False)
```

```python
import functools

import jax
import jax.numpy as jnp
from jax import lax
from jax.experimental import pallas as pl
from jax.experimental.pallas import tpu as pltpu
from jax.sharding import PartitionSpec as P

MESH = pl.DeviceIdType.MESH
CHUNK = 32
GROUP = 64 // CHUNK
LEAD = 96 // CHUNK
HALF = CHUNK // 2
LAG = 80 // CHUNK
HEAD = 64 // CHUNK
NEXT = 256 // CHUNK
BLOCK = 256
HOLD = 23
WARM = 96 // CHUNK


def kernel(n_x, n_y, a_hbm, b_hbm, c_ref, a_rem, b_full, a_loc, a_sem, b_sem, x_send, x_recv, y_send, y_recv, d_send, d_recv, y_ready, d_ready):
    layer = lax.axis_index('dep')
    col = lax.axis_index('col')
    row = lax.axis_index('row')
    rows = a_loc.shape[0]
    width = b_full.shape[2]
    x_peer = (layer, 1 - col, row)
    y_peer = (1 - layer, col, row)
    d_peer = (layer, col, 1 - row)

    barrier = pltpu.get_barrier_semaphore()
    pl.semaphore_signal(barrier, inc=1, device_id=x_peer, device_id_type=MESH)

    @pl.when(layer == 0)
    def _():
        pl.semaphore_signal(barrier, inc=1, device_id=y_peer, device_id_type=MESH)

    @pl.when(row == 1)
    def _():
        pl.semaphore_signal(barrier, inc=1, device_id=d_peer, device_id_type=MESH)

    def place(owner, idx, count):
        start = idx * CHUNK + owner * (rows - (2 * idx + count) * CHUNK)
        return pl.ds(pl.multiple_of(start, CHUNK), count * CHUNK)

    def half(owner, idx):
        start = idx * CHUNK
        return pl.ds(pl.multiple_of(start + owner * (rows - 2 * start - HALF), HALF), HALF)

    def load_a(idx, count, sem):
        sl = place(layer, idx, count)
        return pltpu.make_async_copy(a_hbm.at[sl], a_loc.at[sl], a_sem.at[sem])

    loads = [load_a(i, 1, i) for i in range(HEAD)]
    loads.append(load_a(HEAD, NEXT - HEAD, HEAD))
    loads.append(load_a(NEXT, rows // CHUNK - NEXT, HEAD + 1))
    load_b = pltpu.make_async_copy(b_hbm.at[:, pl.ds(pl.multiple_of(layer * width, 128), width)], b_full.at[row], b_sem)

    def send_x(idx):
        sl = place(layer, idx, 1)
        return pltpu.make_async_remote_copy(
            src_ref=a_hbm.at[sl], dst_ref=a_rem.at[sl], send_sem=x_send.at[idx], recv_sem=x_recv.at[idx],
            device_id=x_peer, device_id_type=MESH)

    def copy_y(owner, idx):
        sl = place(owner, idx, 1)
        return pltpu.make_async_remote_copy(
            src_ref=a_rem.at[sl], dst_ref=a_rem.at[sl], send_sem=y_send.at[idx], recv_sem=y_recv.at[idx],
            device_id=y_peer, device_id_type=MESH)

    def part_x(start, sem):
        sl = pl.ds(pl.multiple_of(start + layer * (rows - 2 * start - HALF), HALF), HALF)
        return pltpu.make_async_remote_copy(
            src_ref=a_hbm.at[sl], dst_ref=a_rem.at[sl], send_sem=x_send.at[sem], recv_sem=x_recv.at[sem],
            device_id=x_peer, device_id_type=MESH)

    parts = [part_x(n_y * CHUNK, n_y), part_x(n_y * CHUNK + HALF, n_x + 1), part_x(n_x * CHUNK, n_x)]

    def half_y(owner):
        sl = half(owner, n_y)
        return pltpu.make_async_remote_copy(
            src_ref=a_rem.at[sl], dst_ref=a_rem.at[sl], send_sem=y_send.at[n_y], recv_sem=y_recv.at[n_y],
            device_id=y_peer, device_id_type=MESH)

    def swap_b(side):
        return pltpu.make_async_remote_copy(
            src_ref=b_full.at[side], dst_ref=b_full.at[side], send_sem=d_send, recv_sem=d_recv,
            device_id=d_peer, device_id_type=MESH)

    for copy in loads[:HEAD + 1]:
        copy.start()
    load_b.start()
    loads[HEAD + 1].start()

    pl.semaphore_wait(barrier, 2 + layer - row)

    for i in range(HEAD):
        send_x(i).start()

    @pl.when(layer == 1)
    def _():
        pl.semaphore_signal(y_ready, inc=1, device_id=y_peer, device_id_type=MESH)

    @pl.when(row == 0)
    def _():
        pl.semaphore_signal(d_ready, inc=1, device_id=d_peer, device_id_type=MESH)

    def launch(i, u):
        send_x(i).start()
        return u

    @pl.when(row == 0)
    def _():
        lax.fori_loop(HEAD, n_y, launch, 0)
        parts[0].start()
        parts[1].start()
        lax.fori_loop(n_y + 1, n_x, launch, 0)
        parts[2].start()

    @pl.when(row == 1)
    def _():
        lax.fori_loop(HEAD, HOLD, launch, 0)

    load_b.wait()

    @pl.when(row == 1)
    def _():
        pl.semaphore_wait(d_ready, 1)

    swap_b(row).start()
    for copy in loads:
        copy.wait()

    @pl.when(layer == 0)
    def _():
        pl.semaphore_wait(y_ready, 1)

    def remote(sl):
        c_ref[sl, :] += jnp.dot(a_rem[sl, :], b_full[1 - col], preferred_element_type=jnp.float32)

    join = WARM + rows // BLOCK
    g_x = n_x // GROUP
    g_y = n_y // GROUP

    def step(i, done):
        x_done, y_done = done

        @pl.when((i < n_x) & ((i != n_y) | (row == 1)))
        def _():
            send_x(i).wait_recv()

        @pl.when(i < n_y)
        def _():
            copy_y(layer, i).start()

        @pl.when((i == n_y) & (row == 0))
        def _():
            parts[0].wait_recv()
            half_y(layer).start()
            parts[1].wait_recv()

        @pl.when((i == n_y) & (row == 1))
        def _():
            copy_y(layer, n_y).start()

        @pl.when((i == HOLD - 1) & (row == 1))
        def _():
            lax.fori_loop(HOLD, n_x, launch, 0)

        @pl.when(i == WARM)
        def _():
            swap_b(1 - row).wait_recv()

        @pl.when((i >= WARM) & (i < join))
        def _():
            sl = pl.ds(pl.multiple_of((i - WARM) * BLOCK, BLOCK), BLOCK)
            c_ref[sl, :] = jnp.dot(a_loc[sl, :], b_full[col], preferred_element_type=jnp.float32)

        is_x = (i >= join) & (x_done < g_x) & ((x_done + 1) * GROUP <= i + 1)
        is_y = (i >= join) & (y_done < g_y) & ((y_done + 1) * GROUP + LAG <= i + 1)

        @pl.when(is_x)
        def _():
            remote(place(layer, x_done * GROUP, GROUP))

        @pl.when(is_y)
        def _():
            for k in range(GROUP):
                copy_y(1 - layer, y_done * GROUP + k).wait_recv()
            remote(place(1 - layer, y_done * GROUP, GROUP))

        return x_done + is_x.astype(jnp.int32), y_done + is_y.astype(jnp.int32)

    lax.fori_loop(0, max(n_x, g_y * GROUP + LAG), step, (0, 0))

    for k in range(g_y * GROUP, n_y):
        copy_y(1 - layer, k).wait_recv()
    @pl.when(row == 0)
    def _():
        parts[2].wait_recv()
        half_y(1 - layer).wait_recv()

    @pl.when(row == 1)
    def _():
        copy_y(1 - layer, n_y).wait_recv()

    lax.fori_loop(0, n_y, lambda i, u: (send_x(i).wait_send(), u)[1], 0)
    lax.fori_loop(n_y + 1, n_x, lambda i, u: (send_x(i).wait_send(), u)[1], 0)
    lax.fori_loop(0, n_y, lambda i, u: (copy_y(layer, i).wait_send(), u)[1], 0)

    @pl.when(row == 0)
    def _():
        for part in parts:
            part.wait_send()
        half_y(layer).wait_send()

    @pl.when(row == 1)
    def _():
        send_x(n_y).wait_send()
        copy_y(layer, n_y).wait_send()

    swap_b(row).wait_send()


def finish(n_x, c_ref, a_rem, b_full, out, last, sem):
    layer = lax.axis_index('dep')
    col = lax.axis_index('col')
    rows = a_rem.shape[0]
    size = GROUP * CHUNK
    count = rows // size
    mine = n_x // GROUP + layer * (count - 1 - 2 * (n_x // GROUP))

    def block(i):
        return pl.ds(pl.multiple_of(i * size, size), size)

    def put(i):
        return pltpu.make_async_copy(c_ref.at[block(i)], out.at[block(i)], sem)

    def put_last():
        return pltpu.make_async_copy(last, out.at[block(mine)], sem)

    def start(i, u):
        @pl.when(i != mine)
        def _():
            put(i).start()

        return u

    lax.fori_loop(0, count, start, 0)
    last[...] = c_ref[block(mine), :] + jnp.dot(a_rem[block(mine), :], b_full[1 - col], preferred_element_type=jnp.float32)
    put_last().start()
    pltpu.make_async_copy(c_ref, out, sem).wait()


def solution(mesh):
    n_dep = mesh.shape['dep']

    def local_product(a_blk, b_blk):
        rows, depth = a_blk.shape
        width = b_blk.shape[1] // n_dep
        n_x = (rows // CHUNK + LEAD - 1) // 2
        n_y = n_x - LEAD
        c, a_rem, b_full = pl.pallas_call(
            functools.partial(kernel, n_x, n_y),
            out_shape=(
                pltpu.VMEM((rows, width), jnp.float32),
                pltpu.VMEM((rows, depth), jnp.bfloat16),
                pltpu.VMEM((2, depth, width), jnp.bfloat16),
            ),
            in_specs=[pl.BlockSpec(memory_space=pltpu.HBM)] * 2,
            out_specs=(pl.BlockSpec(memory_space=pltpu.VMEM),) * 3,
            scratch_shapes=[
                pltpu.VMEM((rows, depth), jnp.bfloat16),
                pltpu.SemaphoreType.DMA((HEAD + 2,)),
                pltpu.SemaphoreType.DMA,
                pltpu.SemaphoreType.DMA((n_x + 2,)),
                pltpu.SemaphoreType.DMA((n_x + 2,)),
                pltpu.SemaphoreType.DMA((n_y + 1,)),
                pltpu.SemaphoreType.DMA((n_y + 1,)),
                pltpu.SemaphoreType.DMA,
                pltpu.SemaphoreType.DMA,
                pltpu.SemaphoreType.REGULAR,
                pltpu.SemaphoreType.REGULAR,
            ],
            compiler_params=pltpu.CompilerParams(collective_id=0, has_side_effects=True, vmem_limit_bytes=40 * 1024 * 1024),
            name='gather_dot',
        )(pltpu.with_memory_space_constraint(a_blk, pltpu.HBM), pltpu.with_memory_space_constraint(b_blk, pltpu.HBM))

        return pl.pallas_call(
            functools.partial(finish, n_x),
            out_shape=pltpu.HBM((rows, width), jnp.float32),
            in_specs=[pl.BlockSpec(memory_space=pltpu.VMEM)] * 3,
            out_specs=pl.BlockSpec(memory_space=pltpu.HBM),
            scratch_shapes=[pltpu.VMEM((GROUP * CHUNK, width), jnp.float32), pltpu.SemaphoreType.DMA],
            compiler_params=pltpu.CompilerParams(vmem_limit_bytes=8 * 1024 * 1024),
            name='finish',
        )(*(pltpu.with_memory_space_constraint(v, pltpu.VMEM) for v in (c, a_rem, b_full)))

    return jax.shard_map(local_product, mesh=mesh, in_specs=(P('row', 'col'), P('row', 'col')), out_specs=P('row', ('col', 'dep')), check_vma=False)
```

```python
import functools

import jax
import jax.numpy as jnp
from jax import lax
from jax.experimental import pallas as pl
from jax.experimental.pallas import tpu as pltpu
from jax.sharding import PartitionSpec as P

MESH = pl.DeviceIdType.MESH
CHUNK = 32
GROUP = 64 // CHUNK
LEAD = 96 // CHUNK
HALF = CHUNK // 2
LAG = 80 // CHUNK
HEAD = 64 // CHUNK
NEXT = 256 // CHUNK
BLOCK = 256
HOLD = 21
WARM = 96 // CHUNK


def kernel(n_x, n_y, a_hbm, b_hbm, c_ref, a_rem, b_full, a_loc, a_sem, b_sem, x_send, x_recv, y_send, y_recv, d_send, d_recv, y_ready, d_ready):
    layer = lax.axis_index('dep')
    col = lax.axis_index('col')
    row = lax.axis_index('row')
    rows = a_loc.shape[0]
    width = b_full.shape[2]
    n_full = n_x - row
    n_pass = n_y + row
    x_peer = (layer, 1 - col, row)
    y_peer = (1 - layer, col, row)
    d_peer = (layer, col, 1 - row)

    barrier = pltpu.get_barrier_semaphore()
    pl.semaphore_signal(barrier, inc=1, device_id=x_peer, device_id_type=MESH)

    @pl.when(layer == 0)
    def _():
        pl.semaphore_signal(barrier, inc=1, device_id=y_peer, device_id_type=MESH)

    @pl.when(row == 1)
    def _():
        pl.semaphore_signal(barrier, inc=1, device_id=d_peer, device_id_type=MESH)

    def place(owner, idx, count):
        start = idx * CHUNK + owner * (rows - (2 * idx + count) * CHUNK)
        return pl.ds(pl.multiple_of(start, CHUNK), count * CHUNK)

    def half(owner, idx):
        start = idx * CHUNK
        return pl.ds(pl.multiple_of(start + owner * (rows - 2 * start - HALF), HALF), HALF)

    def load_a(idx, count, sem):
        sl = place(layer, idx, count)
        return pltpu.make_async_copy(a_hbm.at[sl], a_loc.at[sl], a_sem.at[sem])

    loads = [load_a(i, 1, i) for i in range(HEAD)]
    loads.append(load_a(HEAD, NEXT - HEAD, HEAD))
    loads.append(load_a(NEXT, rows // CHUNK - NEXT, HEAD + 1))
    load_b = pltpu.make_async_copy(b_hbm.at[:, pl.ds(pl.multiple_of(layer * width, 128), width)], b_full.at[row], b_sem)

    def send_x(idx):
        sl = place(layer, idx, 1)
        return pltpu.make_async_remote_copy(
            src_ref=a_hbm.at[sl], dst_ref=a_rem.at[sl], send_sem=x_send.at[idx], recv_sem=x_recv.at[idx],
            device_id=x_peer, device_id_type=MESH)

    def copy_y(owner, idx):
        sl = place(owner, idx, 1)
        return pltpu.make_async_remote_copy(
            src_ref=a_rem.at[sl], dst_ref=a_rem.at[sl], send_sem=y_send.at[idx], recv_sem=y_recv.at[idx],
            device_id=y_peer, device_id_type=MESH)

    half_x = pltpu.make_async_remote_copy(
        src_ref=a_hbm.at[half(layer, n_full)], dst_ref=a_rem.at[half(layer, n_full)], send_sem=x_send.at[n_full], recv_sem=x_recv.at[n_full],
        device_id=x_peer, device_id_type=MESH)

    def half_y(owner):
        sl = half(owner, n_pass)
        return pltpu.make_async_remote_copy(
            src_ref=a_rem.at[sl], dst_ref=a_rem.at[sl], send_sem=y_send.at[n_pass], recv_sem=y_recv.at[n_pass],
            device_id=y_peer, device_id_type=MESH)

    def swap_b(side):
        return pltpu.make_async_remote_copy(
            src_ref=b_full.at[side], dst_ref=b_full.at[side], send_sem=d_send, recv_sem=d_recv,
            device_id=d_peer, device_id_type=MESH)

    for copy in loads[:HEAD + 1]:
        copy.start()
    load_b.start()
    loads[HEAD + 1].start()

    pl.semaphore_wait(barrier, 2 + layer - row)

    for i in range(HEAD):
        send_x(i).start()

    @pl.when(layer == 1)
    def _():
        pl.semaphore_signal(y_ready, inc=1, device_id=y_peer, device_id_type=MESH)

    @pl.when(row == 0)
    def _():
        pl.semaphore_signal(d_ready, inc=1, device_id=d_peer, device_id_type=MESH)

    def launch(i, u):
        send_x(i).start()
        return u

    first_out = jnp.where(row == 0, n_full, HOLD)
    lax.fori_loop(HEAD, first_out, launch, 0)

    @pl.when(row == 0)
    def _():
        half_x.start()

    load_b.wait()

    @pl.when(row == 1)
    def _():
        pl.semaphore_wait(d_ready, 1)

    swap_b(row).start()
    for copy in loads:
        copy.wait()

    @pl.when(layer == 0)
    def _():
        pl.semaphore_wait(y_ready, 1)

    def remote(sl):
        c_ref[sl, :] += jnp.dot(a_rem[sl, :], b_full[1 - col], preferred_element_type=jnp.float32)

    join = WARM + rows // BLOCK
    g_x = n_x // GROUP
    g_y = n_y // GROUP

    def step(i, done):
        x_done, y_done = done

        @pl.when(i < n_full)
        def _():
            send_x(i).wait_recv()

        @pl.when(i < n_pass)
        def _():
            copy_y(layer, i).start()

        @pl.when(i == n_pass)
        def _():
            half_y(layer).start()

        @pl.when((i == HOLD - 1) & (row == 1))
        def _():
            lax.fori_loop(first_out, n_full, launch, 0)
            half_x.start()

        @pl.when(i == WARM)
        def _():
            swap_b(1 - row).wait_recv()

        @pl.when((i >= WARM) & (i < join))
        def _():
            sl = pl.ds(pl.multiple_of((i - WARM) * BLOCK, BLOCK), BLOCK)
            c_ref[sl, :] = jnp.dot(a_loc[sl, :], b_full[col], preferred_element_type=jnp.float32)

        is_x = (i >= join) & (x_done < g_x) & ((x_done + 1) * GROUP <= i + 1)
        is_y = (i >= join) & (y_done < g_y) & ((y_done + 1) * GROUP + LAG <= i + 1)

        @pl.when(is_x)
        def _():
            remote(place(layer, x_done * GROUP, GROUP))

        @pl.when(is_y)
        def _():
            for k in range(GROUP):
                copy_y(1 - layer, y_done * GROUP + k).wait_recv()
            remote(place(1 - layer, y_done * GROUP, GROUP))

        return x_done + is_x.astype(jnp.int32), y_done + is_y.astype(jnp.int32)

    lax.fori_loop(0, max(n_x, g_y * GROUP + LAG), step, (0, 0))

    lax.fori_loop(g_y * GROUP, n_pass, lambda i, u: (copy_y(1 - layer, i).wait_recv(), u)[1], 0)
    half_x.wait_recv()
    half_y(1 - layer).wait_recv()

    lax.fori_loop(0, n_full, lambda i, u: (send_x(i).wait_send(), u)[1], 0)
    lax.fori_loop(0, n_pass, lambda i, u: (copy_y(layer, i).wait_send(), u)[1], 0)
    half_x.wait_send()
    half_y(layer).wait_send()
    swap_b(row).wait_send()


def finish(n_x, c_ref, a_rem, b_full, out, last, sem):
    layer = lax.axis_index('dep')
    col = lax.axis_index('col')
    rows = a_rem.shape[0]
    size = GROUP * CHUNK
    count = rows // size
    mine = n_x // GROUP + layer * (count - 1 - 2 * (n_x // GROUP))

    def block(i):
        return pl.ds(pl.multiple_of(i * size, size), size)

    def put(i):
        return pltpu.make_async_copy(c_ref.at[block(i)], out.at[block(i)], sem)

    def put_last():
        return pltpu.make_async_copy(last, out.at[block(mine)], sem)

    def start(i, u):
        @pl.when(i != mine)
        def _():
            put(i).start()

        return u

    lax.fori_loop(0, count, start, 0)
    last[...] = c_ref[block(mine), :] + jnp.dot(a_rem[block(mine), :], b_full[1 - col], preferred_element_type=jnp.float32)
    put_last().start()
    pltpu.make_async_copy(c_ref, out, sem).wait()


def solution(mesh):
    n_dep = mesh.shape['dep']

    def local_product(a_blk, b_blk):
        rows, depth = a_blk.shape
        width = b_blk.shape[1] // n_dep
        n_x = (rows // CHUNK + LEAD - 1) // 2
        n_y = n_x - LEAD
        c, a_rem, b_full = pl.pallas_call(
            functools.partial(kernel, n_x, n_y),
            out_shape=(
                pltpu.VMEM((rows, width), jnp.float32),
                pltpu.VMEM((rows, depth), jnp.bfloat16),
                pltpu.VMEM((2, depth, width), jnp.bfloat16),
            ),
            in_specs=[pl.BlockSpec(memory_space=pltpu.HBM)] * 2,
            out_specs=(pl.BlockSpec(memory_space=pltpu.VMEM),) * 3,
            scratch_shapes=[
                pltpu.VMEM((rows, depth), jnp.bfloat16),
                pltpu.SemaphoreType.DMA((HEAD + 2,)),
                pltpu.SemaphoreType.DMA,
                pltpu.SemaphoreType.DMA((n_x + 1,)),
                pltpu.SemaphoreType.DMA((n_x + 1,)),
                pltpu.SemaphoreType.DMA((n_y + 2,)),
                pltpu.SemaphoreType.DMA((n_y + 2,)),
                pltpu.SemaphoreType.DMA,
                pltpu.SemaphoreType.DMA,
                pltpu.SemaphoreType.REGULAR,
                pltpu.SemaphoreType.REGULAR,
            ],
            compiler_params=pltpu.CompilerParams(collective_id=0, has_side_effects=True, vmem_limit_bytes=40 * 1024 * 1024),
            name='gather_dot',
        )(pltpu.with_memory_space_constraint(a_blk, pltpu.HBM), pltpu.with_memory_space_constraint(b_blk, pltpu.HBM))

        return pl.pallas_call(
            functools.partial(finish, n_x),
            out_shape=pltpu.HBM((rows, width), jnp.float32),
            in_specs=[pl.BlockSpec(memory_space=pltpu.VMEM)] * 3,
            out_specs=pl.BlockSpec(memory_space=pltpu.HBM),
            scratch_shapes=[pltpu.VMEM((GROUP * CHUNK, width), jnp.float32), pltpu.SemaphoreType.DMA],
            compiler_params=pltpu.CompilerParams(vmem_limit_bytes=8 * 1024 * 1024),
            name='finish',
        )(*(pltpu.with_memory_space_constraint(v, pltpu.VMEM) for v in (c, a_rem, b_full)))

    return jax.shard_map(local_product, mesh=mesh, in_specs=(P('row', 'col'), P('row', 'col')), out_specs=P('row', ('col', 'dep')), check_vma=False)
```

```python
import functools

import jax
import jax.numpy as jnp
from jax import lax
from jax.experimental import pallas as pl
from jax.experimental.pallas import tpu as pltpu
from jax.sharding import PartitionSpec as P

MESH = pl.DeviceIdType.MESH
CHUNK = 32
GROUP = 64 // CHUNK
LEAD = 64 // CHUNK
LAG = 80 // CHUNK
HEAD = 64 // CHUNK
NEXT = 256 // CHUNK
BLOCK = 256
HOLD = 21
WARM = 96 // CHUNK


def kernel(n_x, n_y, a_hbm, b_hbm, c_ref, a_rem, b_full, a_loc, a_sem, b_sem, x_send, x_recv, y_send, y_recv, d_send, d_recv, y_ready, d_ready):
    layer = lax.axis_index('dep')
    col = lax.axis_index('col')
    row = lax.axis_index('row')
    rows = a_loc.shape[0]
    width = b_full.shape[2]
    x_peer = (layer, 1 - col, row)
    y_peer = (1 - layer, col, row)
    d_peer = (layer, col, 1 - row)

    barrier = pltpu.get_barrier_semaphore()
    pl.semaphore_signal(barrier, inc=1, device_id=x_peer, device_id_type=MESH)

    @pl.when(layer == 0)
    def _():
        pl.semaphore_signal(barrier, inc=1, device_id=y_peer, device_id_type=MESH)

    @pl.when(row == 1)
    def _():
        pl.semaphore_signal(barrier, inc=1, device_id=d_peer, device_id_type=MESH)

    def place(owner, idx, count):
        start = idx * CHUNK + owner * (rows - (2 * idx + count) * CHUNK)
        return pl.ds(pl.multiple_of(start, CHUNK), count * CHUNK)

    def load_a(idx, count, sem):
        sl = place(layer, idx, count)
        return pltpu.make_async_copy(a_hbm.at[sl], a_loc.at[sl], a_sem.at[sem])

    loads = [load_a(i, 1, i) for i in range(HEAD)]
    loads.append(load_a(HEAD, NEXT - HEAD, HEAD))
    loads.append(load_a(NEXT, rows // CHUNK - NEXT, HEAD + 1))
    load_b = pltpu.make_async_copy(b_hbm.at[:, pl.ds(pl.multiple_of(layer * width, 128), width)], b_full.at[row], b_sem)

    def send_x(idx):
        sl = place(layer, idx, 1)
        return pltpu.make_async_remote_copy(
            src_ref=a_hbm.at[sl], dst_ref=a_rem.at[sl], send_sem=x_send.at[idx], recv_sem=x_recv.at[idx],
            device_id=x_peer, device_id_type=MESH)

    def copy_y(owner, idx):
        sl = place(owner, idx, 1)
        return pltpu.make_async_remote_copy(
            src_ref=a_rem.at[sl], dst_ref=a_rem.at[sl], send_sem=y_send.at[idx], recv_sem=y_recv.at[idx],
            device_id=y_peer, device_id_type=MESH)

    def swap_b(half):
        return pltpu.make_async_remote_copy(
            src_ref=b_full.at[half], dst_ref=b_full.at[half], send_sem=d_send, recv_sem=d_recv,
            device_id=d_peer, device_id_type=MESH)

    for copy in loads[:HEAD + 1]:
        copy.start()
    load_b.start()
    loads[HEAD + 1].start()

    pl.semaphore_wait(barrier, 2 + layer - row)

    for i in range(HEAD):
        send_x(i).start()

    @pl.when(layer == 1)
    def _():
        pl.semaphore_signal(y_ready, inc=1, device_id=y_peer, device_id_type=MESH)

    @pl.when(row == 0)
    def _():
        pl.semaphore_signal(d_ready, inc=1, device_id=d_peer, device_id_type=MESH)

    def launch(i, u):
        send_x(i).start()
        return u

    first_out = jnp.where(row == 0, n_x, HOLD)
    lax.fori_loop(HEAD, first_out, launch, 0)
    load_b.wait()

    @pl.when(row == 1)
    def _():
        pl.semaphore_wait(d_ready, 1)

    swap_b(row).start()
    for copy in loads:
        copy.wait()

    @pl.when(layer == 0)
    def _():
        pl.semaphore_wait(y_ready, 1)

    def remote(sl):
        c_ref[sl, :] += jnp.dot(a_rem[sl, :], b_full[1 - col], preferred_element_type=jnp.float32)

    join = WARM + rows // BLOCK
    g_x = n_x // GROUP
    g_y = n_y // GROUP

    def step(i, done):
        x_done, y_done = done

        @pl.when(i < n_x)
        def _():
            send_x(i).wait_recv()

        @pl.when(i < n_y)
        def _():
            copy_y(layer, i).start()

        @pl.when((i == HOLD - 1) & (row == 1))
        def _():
            lax.fori_loop(HOLD, n_x, launch, 0)

        @pl.when(i == WARM)
        def _():
            swap_b(1 - row).wait_recv()

        @pl.when((i >= WARM) & (i < join))
        def _():
            sl = pl.ds(pl.multiple_of((i - WARM) * BLOCK, BLOCK), BLOCK)
            c_ref[sl, :] = jnp.dot(a_loc[sl, :], b_full[col], preferred_element_type=jnp.float32)

        is_x = (i >= join) & (x_done < g_x) & ((x_done + 1) * GROUP <= i + 1)
        is_y = (i >= join) & (y_done < g_y) & ((y_done + 1) * GROUP + LAG <= i + 1)

        @pl.when(is_x)
        def _():
            remote(place(layer, x_done * GROUP, GROUP))

        @pl.when(is_y)
        def _():
            for k in range(GROUP):
                copy_y(1 - layer, y_done * GROUP + k).wait_recv()
            remote(place(1 - layer, y_done * GROUP, GROUP))

        return x_done + is_x.astype(jnp.int32), y_done + is_y.astype(jnp.int32)

    lax.fori_loop(0, max(n_x, g_y * GROUP + LAG), step, (0, 0))

    for k in range(g_y * GROUP, n_y):
        copy_y(1 - layer, k).wait_recv()
    lax.fori_loop(0, n_x, lambda i, u: (send_x(i).wait_send(), u)[1], 0)
    lax.fori_loop(0, n_y, lambda i, u: (copy_y(layer, i).wait_send(), u)[1], 0)
    swap_b(row).wait_send()


def finish(n_x, c_ref, a_rem, b_full, out, last, sem):
    layer = lax.axis_index('dep')
    col = lax.axis_index('col')
    rows = a_rem.shape[0]
    size = GROUP * CHUNK
    count = rows // size
    mine = n_x // GROUP + layer * (count - 1 - 2 * (n_x // GROUP))

    def block(i):
        return pl.ds(pl.multiple_of(i * size, size), size)

    def put(i):
        return pltpu.make_async_copy(c_ref.at[block(i)], out.at[block(i)], sem)

    def put_last():
        return pltpu.make_async_copy(last, out.at[block(mine)], sem)

    def start(i, u):
        @pl.when(i != mine)
        def _():
            put(i).start()

        return u

    lax.fori_loop(0, count, start, 0)
    last[...] = c_ref[block(mine), :] + jnp.dot(a_rem[block(mine), :], b_full[1 - col], preferred_element_type=jnp.float32)
    put_last().start()
    pltpu.make_async_copy(c_ref, out, sem).wait()


def solution(mesh):
    n_dep = mesh.shape['dep']

    def local_product(a_blk, b_blk):
        rows, depth = a_blk.shape
        width = b_blk.shape[1] // n_dep
        n_x = (rows // CHUNK + LEAD) // 2
        n_y = n_x - LEAD
        c, a_rem, b_full = pl.pallas_call(
            functools.partial(kernel, n_x, n_y),
            out_shape=(
                pltpu.VMEM((rows, width), jnp.float32),
                pltpu.VMEM((rows, depth), jnp.bfloat16),
                pltpu.VMEM((2, depth, width), jnp.bfloat16),
            ),
            in_specs=[pl.BlockSpec(memory_space=pltpu.HBM)] * 2,
            out_specs=(pl.BlockSpec(memory_space=pltpu.VMEM),) * 3,
            scratch_shapes=[
                pltpu.VMEM((rows, depth), jnp.bfloat16),
                pltpu.SemaphoreType.DMA((HEAD + 2,)),
                pltpu.SemaphoreType.DMA,
                pltpu.SemaphoreType.DMA((n_x,)),
                pltpu.SemaphoreType.DMA((n_x,)),
                pltpu.SemaphoreType.DMA((n_y,)),
                pltpu.SemaphoreType.DMA((n_y,)),
                pltpu.SemaphoreType.DMA,
                pltpu.SemaphoreType.DMA,
                pltpu.SemaphoreType.REGULAR,
                pltpu.SemaphoreType.REGULAR,
            ],
            compiler_params=pltpu.CompilerParams(collective_id=0, has_side_effects=True, vmem_limit_bytes=40 * 1024 * 1024),
            name='gather_dot',
        )(pltpu.with_memory_space_constraint(a_blk, pltpu.HBM), pltpu.with_memory_space_constraint(b_blk, pltpu.HBM))

        return pl.pallas_call(
            functools.partial(finish, n_x),
            out_shape=pltpu.HBM((rows, width), jnp.float32),
            in_specs=[pl.BlockSpec(memory_space=pltpu.VMEM)] * 3,
            out_specs=pl.BlockSpec(memory_space=pltpu.HBM),
            scratch_shapes=[pltpu.VMEM((GROUP * CHUNK, width), jnp.float32), pltpu.SemaphoreType.DMA],
            compiler_params=pltpu.CompilerParams(vmem_limit_bytes=8 * 1024 * 1024),
            name='finish',
        )(*(pltpu.with_memory_space_constraint(v, pltpu.VMEM) for v in (c, a_rem, b_full)))

    return jax.shard_map(local_product, mesh=mesh, in_specs=(P('row', 'col'), P('row', 'col')), out_specs=P('row', ('col', 'dep')), check_vma=False)
```

```python
import functools

import jax
import jax.numpy as jnp
from jax import lax
from jax.experimental import pallas as pl
from jax.experimental.pallas import tpu as pltpu
from jax.sharding import PartitionSpec as P

MESH = pl.DeviceIdType.MESH
CHUNK = 32
GROUP = 64 // CHUNK
LEAD = 64 // CHUNK
LAG = 80 // CHUNK
HEAD = 64 // CHUNK
NEXT = 256 // CHUNK
BLOCK = 256
HOLD = 19
WARM = 96 // CHUNK


def kernel(n_x, n_y, a_hbm, b_hbm, c_ref, a_rem, b_full, a_loc, a_sem, b_sem, x_send, x_recv, y_send, y_recv, d_send, d_recv, y_ready, d_ready):
    layer = lax.axis_index('dep')
    col = lax.axis_index('col')
    row = lax.axis_index('row')
    rows = a_loc.shape[0]
    width = b_full.shape[2]
    x_peer = (layer, 1 - col, row)
    y_peer = (1 - layer, col, row)
    d_peer = (layer, col, 1 - row)

    barrier = pltpu.get_barrier_semaphore()
    pl.semaphore_signal(barrier, inc=1, device_id=x_peer, device_id_type=MESH)

    @pl.when(layer == 0)
    def _():
        pl.semaphore_signal(barrier, inc=1, device_id=y_peer, device_id_type=MESH)

    @pl.when(row == 1)
    def _():
        pl.semaphore_signal(barrier, inc=1, device_id=d_peer, device_id_type=MESH)

    def place(owner, idx, count):
        start = idx * CHUNK + owner * (rows - (2 * idx + count) * CHUNK)
        return pl.ds(pl.multiple_of(start, CHUNK), count * CHUNK)

    def load_a(idx, count, sem):
        sl = place(layer, idx, count)
        return pltpu.make_async_copy(a_hbm.at[sl], a_loc.at[sl], a_sem.at[sem])

    loads = [load_a(i, 1, i) for i in range(HEAD)]
    loads.append(load_a(HEAD, NEXT - HEAD, HEAD))
    loads.append(load_a(NEXT, rows // CHUNK - NEXT, HEAD + 1))
    load_b = pltpu.make_async_copy(b_hbm.at[:, pl.ds(pl.multiple_of(layer * width, 128), width)], b_full.at[row], b_sem)

    def send_x(idx):
        sl = place(layer, idx, 1)
        return pltpu.make_async_remote_copy(
            src_ref=a_hbm.at[sl], dst_ref=a_rem.at[sl], send_sem=x_send.at[idx], recv_sem=x_recv.at[idx],
            device_id=x_peer, device_id_type=MESH)

    def copy_y(owner, idx):
        sl = place(owner, idx, 1)
        return pltpu.make_async_remote_copy(
            src_ref=a_rem.at[sl], dst_ref=a_rem.at[sl], send_sem=y_send.at[idx], recv_sem=y_recv.at[idx],
            device_id=y_peer, device_id_type=MESH)

    def swap_b(half):
        return pltpu.make_async_remote_copy(
            src_ref=b_full.at[half], dst_ref=b_full.at[half], send_sem=d_send, recv_sem=d_recv,
            device_id=d_peer, device_id_type=MESH)

    for copy in loads[:HEAD + 1]:
        copy.start()
    load_b.start()
    loads[HEAD + 1].start()

    pl.semaphore_wait(barrier, 2 + layer - row)

    for i in range(HEAD):
        send_x(i).start()

    @pl.when(layer == 1)
    def _():
        pl.semaphore_signal(y_ready, inc=1, device_id=y_peer, device_id_type=MESH)

    @pl.when(row == 0)
    def _():
        pl.semaphore_signal(d_ready, inc=1, device_id=d_peer, device_id_type=MESH)

    def launch(i, u):
        send_x(i).start()
        return u

    first_out = jnp.where(row == 0, n_x, HOLD)
    lax.fori_loop(HEAD, first_out, launch, 0)
    load_b.wait()

    @pl.when(row == 1)
    def _():
        pl.semaphore_wait(d_ready, 1)

    swap_b(row).start()
    for copy in loads:
        copy.wait()

    @pl.when(layer == 0)
    def _():
        pl.semaphore_wait(y_ready, 1)

    def remote(sl):
        c_ref[sl, :] += jnp.dot(a_rem[sl, :], b_full[1 - col], preferred_element_type=jnp.float32)

    join = WARM + rows // BLOCK
    g_x = n_x // GROUP
    g_y = n_y // GROUP

    def step(i, done):
        x_done, y_done = done

        @pl.when(i < n_x)
        def _():
            send_x(i).wait_recv()

        @pl.when(i < n_y)
        def _():
            copy_y(layer, i).start()

        @pl.when((i == HOLD - 1) & (row == 1))
        def _():
            lax.fori_loop(HOLD, n_x, launch, 0)

        @pl.when(i == WARM)
        def _():
            swap_b(1 - row).wait_recv()

        @pl.when((i >= WARM) & (i < join))
        def _():
            sl = pl.ds(pl.multiple_of((i - WARM) * BLOCK, BLOCK), BLOCK)
            c_ref[sl, :] = jnp.dot(a_loc[sl, :], b_full[col], preferred_element_type=jnp.float32)

        is_x = (i >= join) & (x_done < g_x) & ((x_done + 1) * GROUP <= i + 1)
        is_y = (i >= join) & (y_done < g_y) & ((y_done + 1) * GROUP + LAG <= i + 1)

        @pl.when(is_x)
        def _():
            remote(place(layer, x_done * GROUP, GROUP))

        @pl.when(is_y)
        def _():
            for k in range(GROUP):
                copy_y(1 - layer, y_done * GROUP + k).wait_recv()
            remote(place(1 - layer, y_done * GROUP, GROUP))

        return x_done + is_x.astype(jnp.int32), y_done + is_y.astype(jnp.int32)

    lax.fori_loop(0, max(n_x, g_y * GROUP + LAG), step, (0, 0))

    for k in range(g_y * GROUP, n_y):
        copy_y(1 - layer, k).wait_recv()
    lax.fori_loop(0, n_x, lambda i, u: (send_x(i).wait_send(), u)[1], 0)
    lax.fori_loop(0, n_y, lambda i, u: (copy_y(layer, i).wait_send(), u)[1], 0)
    swap_b(row).wait_send()


def finish(n_x, c_ref, a_rem, b_full, out, last, sem):
    layer = lax.axis_index('dep')
    col = lax.axis_index('col')
    rows = a_rem.shape[0]
    size = GROUP * CHUNK
    count = rows // size
    mine = n_x // GROUP + layer * (count - 1 - 2 * (n_x // GROUP))

    def block(i):
        return pl.ds(pl.multiple_of(i * size, size), size)

    def put(i):
        return pltpu.make_async_copy(c_ref.at[block(i)], out.at[block(i)], sem)

    def put_last():
        return pltpu.make_async_copy(last, out.at[block(mine)], sem)

    def start(i, u):
        @pl.when(i != mine)
        def _():
            put(i).start()

        return u

    lax.fori_loop(0, count, start, 0)
    last[...] = c_ref[block(mine), :] + jnp.dot(a_rem[block(mine), :], b_full[1 - col], preferred_element_type=jnp.float32)
    put_last().start()
    pltpu.make_async_copy(c_ref, out, sem).wait()


def solution(mesh):
    n_dep = mesh.shape['dep']

    def local_product(a_blk, b_blk):
        rows, depth = a_blk.shape
        width = b_blk.shape[1] // n_dep
        n_x = (rows // CHUNK + LEAD) // 2
        n_y = n_x - LEAD
        c, a_rem, b_full = pl.pallas_call(
            functools.partial(kernel, n_x, n_y),
            out_shape=(
                pltpu.VMEM((rows, width), jnp.float32),
                pltpu.VMEM((rows, depth), jnp.bfloat16),
                pltpu.VMEM((2, depth, width), jnp.bfloat16),
            ),
            in_specs=[pl.BlockSpec(memory_space=pltpu.HBM)] * 2,
            out_specs=(pl.BlockSpec(memory_space=pltpu.VMEM),) * 3,
            scratch_shapes=[
                pltpu.VMEM((rows, depth), jnp.bfloat16),
                pltpu.SemaphoreType.DMA((HEAD + 2,)),
                pltpu.SemaphoreType.DMA,
                pltpu.SemaphoreType.DMA((n_x,)),
                pltpu.SemaphoreType.DMA((n_x,)),
                pltpu.SemaphoreType.DMA((n_y,)),
                pltpu.SemaphoreType.DMA((n_y,)),
                pltpu.SemaphoreType.DMA,
                pltpu.SemaphoreType.DMA,
                pltpu.SemaphoreType.REGULAR,
                pltpu.SemaphoreType.REGULAR,
            ],
            compiler_params=pltpu.CompilerParams(collective_id=0, has_side_effects=True, vmem_limit_bytes=40 * 1024 * 1024),
            name='gather_dot',
        )(pltpu.with_memory_space_constraint(a_blk, pltpu.HBM), pltpu.with_memory_space_constraint(b_blk, pltpu.HBM))

        return pl.pallas_call(
            functools.partial(finish, n_x),
            out_shape=pltpu.HBM((rows, width), jnp.float32),
            in_specs=[pl.BlockSpec(memory_space=pltpu.VMEM)] * 3,
            out_specs=pl.BlockSpec(memory_space=pltpu.HBM),
            scratch_shapes=[pltpu.VMEM((GROUP * CHUNK, width), jnp.float32), pltpu.SemaphoreType.DMA],
            compiler_params=pltpu.CompilerParams(vmem_limit_bytes=8 * 1024 * 1024),
            name='finish',
        )(*(pltpu.with_memory_space_constraint(v, pltpu.VMEM) for v in (c, a_rem, b_full)))

    return jax.shard_map(local_product, mesh=mesh, in_specs=(P('row', 'col'), P('row', 'col')), out_specs=P('row', ('col', 'dep')), check_vma=False)
```
